32 devices in a mesh: beads: 2 (over y), atoms: 4 (over z), kvec: 4 (over x, core).
Axes of the slice: x: 2, y: 2, z: 4, core: 2. Of those that a mesh axis runs over, the one named last changes fastest.
Arguments:
- lattice: int32 [3, 1024], P(None, ('atoms', 'kvec')), may hold values from -20 to 20, as said below
- positions: float32 [3, 8192], P(None, ('beads', 'atoms', 'kvec')), parts along dimension 1, may hold values from 0 to 1
- cotangent: bfloat16 [8192, 128], P(('beads', 'atoms', 'kvec')), parts along dimension 0, may hold values from -6 to 6
- filters: float32 [1024, 128], P(('atoms', 'kvec')), may hold values from 0.1 to 2
- saved_factor: float32 [2, 2048, 128], P(None, ('beads', 'atoms', 'kvec')), parts along dimension 1, may hold values from -6 to 6
Outputs:
- node_grad: bfloat16 [8192, 128], P(('beads', 'atoms', 'kvec')), parts along dimension 0
- filter_grad: float32 [2048, 128], P(('beads', 'atoms', 'kvec')), parts along dimension 0
The draws below stay inside these ranges and needn't reach their ends.
There are 2 independent parts, one for each index of `beads`. The reference program is written for one: setup_inputs(seed, part) draws one part's arguments, and reference() takes and returns one part's arrays. A program takes and returns all parts, laid end to end along the dimension named above; an argument that names none is the same for every part. Nothing has to cross between parts.
Inputs may be any that keep to these rules, and one draw needn't show every extreme that they name: `lattice`: the columns are 1024 distinct integer vectors of length at most 20, all in one half-space (no vector appears together with its negative), in random order.
All inputs are finite; a program needn't handle non-finite values.
Results may differ from the reference program's by a relative error of at most 0.0056.
Values may be sent and summed in bfloat16 or wider, within the bound.
No kernel may reach another device: no remote copies, remote signals or barrier semaphores. Data moves between devices by JAX's collectives and lax.ppermute only.
A program may use at most 64 MiB of HBM per device.

```python
import math
import jax
import jax.numpy as jnp
from jax import lax

C = 128
NATOM = 4096
NWAVE = 1024


def draw_lattice(key, part):
    radius = 20
    breadth = 2 * radius + 1
    all_cells = breadth * breadth * breadth
    indices = jnp.arange(all_cells, dtype=jnp.int32)
    along_x = indices % breadth - radius
    along_y = indices // breadth % breadth - radius
    along_z = indices // (breadth * breadth) - radius
    inside = along_x * along_x + along_y * along_y + along_z * along_z <= radius * radius
    upper_half = (along_z > 0) | (along_z == 0) & ((along_y > 0) | (along_y == 0) & (along_x > 0))
    chosen_flag = (inside & upper_half).astype(jnp.int32)
    shuffled = jax.random.permutation(jax.random.fold_in(key, 7), all_cells).astype(jnp.int32)
    flagged = chosen_flag[shuffled]
    ranked = jnp.argsort(1 - flagged, stable=True)
    chosen = shuffled[ranked][:NWAVE]
    return jnp.stack([along_x[chosen], along_y[chosen], along_z[chosen]], 0).astype(jnp.int32)


def block_scale(stream_key, extent, cuts, least, top_value):
    factor_of = 1.0
    for axis_at, blocks in cuts:
        heights = jax.random.uniform(jax.random.fold_in(jax.random.fold_in(stream_key, 6), axis_at), (blocks,), jnp.float32, least / len(cuts), top_value / len(cuts))
        factor_of = factor_of * jnp.repeat(jnp.exp(heights), extent[axis_at] // blocks).reshape((-1,) + (1,) * (len(extent) - 1 - axis_at))
    return factor_of


def gaussian(rng, shape, spread, most, shards=(), kind=jnp.bfloat16):
    result = spread * jax.random.normal(rng, shape, jnp.float32)
    if shards:
        result = result * block_scale(rng, shape, shards, -0.22, 0.18)
    return jnp.clip(result, -most, most).astype(kind)


def setup_inputs(seed: int = 0, part: int = 0) -> dict:
    splits = jax.random.split(jax.random.key(seed), 6)
    part_keys = jax.random.split(jax.random.fold_in(splits[5], part), 6)
    return {
        "lattice": draw_lattice(jax.random.fold_in(splits[5], 71), part),
        "positions": jnp.clip(1.0 * jax.random.uniform(part_keys[1], (3, NATOM), jnp.float32) ** block_scale(part_keys[1], (3, NATOM), ((1, 16),), -0.2, 0.2), 0.0, 1.0),
        "cotangent": gaussian(part_keys[2], (NATOM, C), 1.0, 6.0, ((0, 16),)),
        "filters": jnp.clip(jnp.exp(math.log(2.0) - 2.9957323 * jax.random.uniform(splits[3], (NWAVE, C), jnp.float32) ** block_scale(splits[3], (NWAVE, C), ((0, 16),), -0.2, 0.2)), 0.1, 2.0),
        "saved_factor": gaussian(part_keys[4], (2, NWAVE, C), 1.0, 6.0, ((1, 16),), jnp.float32),
    }


two_pi = 2.0 * math.pi

def trig_tile(pos, wave):
    phase = two_pi * (pos[0][:, None] * wave[0][None, :] + pos[1][:, None] * wave[1][None, :] + pos[2][:, None] * wave[2][None, :])
    return jnp.concatenate([jnp.cos(phase), jnp.sin(phase)], 1).astype(jnp.bfloat16)

def reference(lattice, positions, cotangent, filters, saved_factor):
    wave = lattice.astype(jnp.float32)
    width = min(1024, NWAVE)
    count = NWAVE // width
    wave_blocks = jnp.transpose(wave.reshape(3, count, width), (1, 0, 2))
    filt_blocks = filters.reshape(count, width, C)
    saved_blocks = jnp.transpose(saved_factor.reshape(2, count, width, C), (1, 0, 2, 3))
    scale_n = 1.0 / math.sqrt(NATOM)
    scale_k = 1.0 / math.sqrt(NWAVE)

    def first(item):
        wv, fl, sv = item
        tile = trig_tile(positions, wv)
        summed = jnp.dot(tile.T, cotangent, preferred_element_type=jnp.float32) * scale_n
        f_re, f_im = (summed[:width], summed[width:])
        fgrad = f_re * sv[0] + f_im * sv[1]
        weighted = jnp.concatenate([fl * f_re, fl * f_im], 0).astype(jnp.bfloat16)
        return (fgrad, weighted)
    fgrads, weighted = lax.map(first, (wave_blocks, filt_blocks, saved_blocks))

    def second(total, item):
        wv, wt = item
        tile = trig_tile(positions, wv)
        return (total + jnp.dot(tile, wt, preferred_element_type=jnp.float32), None)
    total, unused = lax.scan(second, jnp.zeros((NATOM, C), jnp.float32), (wave_blocks, weighted))
    node_grad = (total * scale_k).astype(jnp.bfloat16)
    return (node_grad, fgrads.reshape(NWAVE, C))
```

```python
import math

import jax
import jax.numpy as jnp
from jax import lax
from jax.experimental import pallas as pl
from jax.experimental.pallas import tpu as pltpu
from jax.sharding import PartitionSpec as P

f32 = jnp.float32
bf16 = jnp.bfloat16


SIN_COEF = None
COS_COEF = None


def _fit():
    import numpy as np

    n = 4001
    t = np.cos(np.pi * (np.arange(n) + 0.5) / n)
    u = (t + 1.0) * 0.125
    r = np.sqrt(u)
    root = math.sqrt(2.0)
    sin_ratio = np.where(r > 1e-9, root * np.sin(np.pi * r) / np.maximum(r, 1e-9), root * np.pi)
    cheb = np.polynomial.chebyshev.Chebyshev
    s = cheb.fit(u, sin_ratio, 4, domain=[0.0, 0.25]).convert(kind=np.polynomial.Polynomial)
    c = cheb.fit(u, root * np.cos(np.pi * r), 4, domain=[0.0, 0.25]).convert(kind=np.polynomial.Polynomial)
    return tuple(float(v) for v in s.coef), tuple(float(v) for v in c.coef)


SIN_COEF, COS_COEF = _fit()


def _horner(coef, u):
    acc = jnp.full_like(u, coef[-1])
    for value in coef[-2::-1]:
        acc = acc * u + value
    return acc


def cos_sin(phase):
    r = phase - jnp.round(phase)
    u = r * r
    s = r * _horner(SIN_COEF, u)
    c = _horner(COS_COEF, u)
    return 1.0 - s * s, s * c


def full_spec(count):
    return [pl.BlockSpec(memory_space=pltpu.VMEM)] * count


def call(body, outs, *args, scratch=()):
    return pl.pallas_call(
        body,
        out_shape=outs,
        in_specs=full_spec(len(args)),
        out_specs=full_spec(len(outs)),
        scratch_shapes=list(scratch),
    )(*args)


def pack_body(lat_ref, pos_ref, cot_ref, fil_ref, zbuf_ref, lbuf_ref):
    natom = cot_ref.shape[0]
    nk = fil_ref.shape[0]
    width = cot_ref.shape[1]
    zbuf_ref[0:natom, :] = cot_ref[...]
    x = pos_ref[...]
    hi = x.astype(bf16).astype(f32)
    rest = x - hi
    mid = rest.astype(bf16).astype(f32)
    low = rest - mid
    zero = jnp.zeros_like(x)
    parts = jnp.concatenate([hi, mid, low, zero, zero, zero[:1]], 0).astype(bf16)
    for j in range(natom // width):
        zbuf_ref[natom + 16 * j : natom + 16 * (j + 1), :] = parts[:, j * width : (j + 1) * width]
    lbuf_ref[0:nk, :] = fil_ref[...]
    row = lax.broadcasted_iota(jnp.int32, (nk, width), 0)
    col = lax.broadcasted_iota(jnp.int32, (nk, width), 1)
    spread = (row == col % nk).astype(bf16)
    lat = lat_ref[...].astype(f32).astype(bf16)
    wide = jnp.dot(lat, spread, preferred_element_type=f32)
    lbuf_ref[nk : nk + 8, :] = jnp.concatenate([wide, wide, wide[:2]], 0)


def factor_body(nz, nq, natom, nk, *refs):
    zb = refs[:nz]
    lb = refs[nz : nz + nq]
    tile_ref, f_ref, fb_ref, acc_ref = refs[nz + nq :]
    width = zb[0].shape[1]
    per = width // nk
    nw = nq * nk
    lane = lax.broadcasted_iota(jnp.int32, (8, width), 1)
    cols = []
    for g in range(nq // per):
        piece = lb[g * per][nk : nk + 8, :]
        for j in range(1, per):
            piece = jnp.where(lane >= j * nk, lb[g * per + j][nk : nk + 8, :], piece)
        cols.append(piece)
    lat = jnp.concatenate(cols, 1)[:3]
    zero = jnp.zeros_like(lat)
    lat9 = jnp.concatenate([lat, lat, lat, zero, zero, zero[:1]], 0).astype(bf16)
    step = 32
    for z in range(nz):
        parts = jnp.concatenate(
            [zb[z][natom + 16 * j : natom + 16 * (j + 1), :] for j in range(natom // width)], 1
        )
        phase = lax.dot_general(parts, lat9, (((0,), (0,)), ((), ())), preferred_element_type=f32)
        for i in range(0, natom, step):
            c, s = cos_sin(phase[i : i + step])
            tile_ref[z * natom + i : z * natom + i + step, 0:nw] = c.astype(bf16)
            tile_ref[z * natom + i : z * natom + i + step, nw : 2 * nw] = s.astype(bf16)
        part = lax.dot_general(
            zb[z][0:natom, :],
            tile_ref[z * natom : (z + 1) * natom, :],
            (((0,), (0,)), ((), ())),
            preferred_element_type=f32,
        )
        if z == 0:
            acc_ref[...] = part
        else:
            acc_ref[...] += part
    total = acc_ref[...].T
    f_ref[...] = total
    fb_ref[...] = total.astype(bf16)


def shuffled(ref, flip, nq, nk):
    rows = [ref[h * nq * nk + (t ^ flip) * nk : h * nq * nk + ((t ^ flip) + 1) * nk, :] for h in range(2) for t in range(nq)]
    return jnp.concatenate(rows, 0).astype(f32)


def pair_body(nq, nk, own_ref, got_ref, f_ref, fb_ref):
    total = own_ref[...] + shuffled(got_ref, 1, nq, nk)
    f_ref[...] = total
    fb_ref[...] = total.astype(bf16)


def node_body(nz, nq, natom, nk, flips, scale, *refs):
    own_ref = refs[0]
    got = refs[1 : 1 + len(flips)]
    lb = refs[1 + len(flips) : 1 + len(flips) + nq]
    tile_ref, saved_ref = refs[1 + len(flips) + nq : 3 + len(flips) + nq]
    grad_ref = refs[3 + len(flips) + nq]
    outs = refs[4 + len(flips) + nq :]
    total = own_ref[...]
    for ref, flip in zip(got, flips):
        total = total + shuffled(ref, flip, nq, nk)
    total = total * scale
    nw = nq * nk
    fil = jnp.concatenate([lb[t][0:nk, :] for t in range(nq)], 0)
    weighted = jnp.concatenate([fil * total[:nw], fil * total[nw:]], 0).astype(bf16)
    grad_ref[...] = total[0:nk] * saved_ref[0] + total[nw : nw + nk] * saved_ref[1]
    for z in range(nz):
        part = jnp.dot(tile_ref[z * natom : (z + 1) * natom, :], weighted, preferred_element_type=f32)
        outs[z][...] = part.astype(outs[z].dtype)


def final_body(scale, *refs):
    total = refs[0][...]
    for ref in refs[1:-1]:
        total = total + ref[...].astype(f32)
    refs[-1][...] = (total * scale).astype(bf16)


def shape(dims, kind):
    return jax.ShapeDtypeStruct(dims, kind)


def local(lattice, positions, cotangent, filters, saved_factor):
    nz = lax.axis_size("atoms")
    nq = lax.axis_size("kvec")
    natom, width = cotangent.shape
    nk = lattice.shape[1]
    nw = nq * nk
    scale_n = 1.0 / math.sqrt(natom * nz * nq)
    scale_k = 1.0 / math.sqrt(nk * nz * nq)

    def swap(value, axis, size, flip):
        return lax.ppermute(value, axis, [(i, i ^ flip) for i in range(size)])

    zbuf, lbuf = call(
        pack_body,
        [shape((natom + 16 * (natom // width), width), bf16), shape((nk + 8, width), f32)],
        lattice,
        positions,
        cotangent,
        filters,
    )
    zb = [zbuf] + [swap(zbuf, "atoms", nz, s) for s in range(1, nz)]
    lb = {0: lbuf}
    for s in range(2, nq, 2):
        lb[s] = swap(lbuf, "kvec", nq, s)
    for s in range(0, nq, 2):
        lb[s + 1] = swap(lb[s], "kvec", nq, 1)
    lb = [lb[s] for s in range(nq)]
    tile, part, part16 = call(
        lambda *refs: factor_body(nz, nq, natom, nk, *refs),
        [shape((nz * natom, 2 * nw), bf16), shape((2 * nw, width), f32), shape((2 * nw, width), bf16)],
        *zb,
        *lb,
        scratch=[pltpu.VMEM((width, 2 * nw), f32)],
    )
    pair, pair16 = call(
        lambda *refs: pair_body(nq, nk, *refs),
        [shape((2 * nw, width), f32), shape((2 * nw, width), bf16)],
        part,
        swap(part16, "kvec", nq, 1),
    )
    flips = list(range(2, nq, 2))
    got = [swap(pair16, "kvec", nq, s) for s in flips]
    filter_grad, *nodes = call(
        lambda *refs: node_body(nz, nq, natom, nk, flips, scale_n, *refs),
        [shape((nk, width), f32), shape((natom, width), f32)] + [shape((natom, width), bf16)] * (nz - 1),
        pair,
        *got,
        *lb,
        tile,
        saved_factor,
    )
    (node_grad,) = call(
        lambda *refs: final_body(scale_k, *refs),
        [shape((natom, width), bf16)],
        nodes[0],
        *[swap(nodes[s], "atoms", nz, s) for s in range(1, nz)],
    )
    return (node_grad, filter_grad)


def solution(mesh):
    in_specs = (
        P(None, ("atoms", "kvec")),
        P(None, ("beads", "atoms", "kvec")),
        P(("beads", "atoms", "kvec"), None),
        P(("atoms", "kvec"), None),
        P(None, ("beads", "atoms", "kvec"), None),
    )
    out_specs = (P(("beads", "atoms", "kvec"), None), P(("beads", "atoms", "kvec"), None))
    return jax.shard_map(local, mesh=mesh, in_specs=in_specs, out_specs=out_specs, check_vma=False)
```

```python
import math

import jax
import jax.numpy as jnp
from jax import lax
from jax.experimental import pallas as pl
from jax.experimental.pallas import tpu as pltpu
from jax.sharding import PartitionSpec as P

f32 = jnp.float32
bf16 = jnp.bfloat16


SIN_COEF = None
COS_COEF = None


def _fit():
    import numpy as np

    n = 4001
    t = np.cos(np.pi * (np.arange(n) + 0.5) / n)
    u = (t + 1.0) * 0.125
    r = np.sqrt(u)
    root = math.sqrt(2.0)
    sin_ratio = np.where(r > 1e-9, root * np.sin(np.pi * r) / np.maximum(r, 1e-9), root * np.pi)
    cheb = np.polynomial.chebyshev.Chebyshev
    s = cheb.fit(u, sin_ratio, 4, domain=[0.0, 0.25]).convert(kind=np.polynomial.Polynomial)
    c = cheb.fit(u, root * np.cos(np.pi * r), 4, domain=[0.0, 0.25]).convert(kind=np.polynomial.Polynomial)
    return tuple(float(v) for v in s.coef), tuple(float(v) for v in c.coef)


SIN_COEF, COS_COEF = _fit()


def _horner(coef, u):
    acc = jnp.full_like(u, coef[-1])
    for value in coef[-2::-1]:
        acc = acc * u + value
    return acc


def cos_sin(phase):
    r = phase - jnp.round(phase)
    u = r * r
    s = r * _horner(SIN_COEF, u)
    c = _horner(COS_COEF, u)
    return 1.0 - s * s, s * c


def full_spec(count):
    return [pl.BlockSpec(memory_space=pltpu.VMEM)] * count


VMEM_BUDGET = 8 * 1024 * 1024


def call(body, outs, *args, scratch=(), keep_args=True, keep_outs=True):
    fits = sum(v.size * v.dtype.itemsize for v in (*outs, *args)) <= VMEM_BUDGET
    if fits and keep_args:
        args = [pltpu.with_memory_space_constraint(arg, pltpu.VMEM) for arg in args]
    if fits and keep_outs:
        outs = [pltpu.VMEM(v.shape, v.dtype) for v in outs]
    return pl.pallas_call(
        body,
        out_shape=outs,
        in_specs=full_spec(len(args)),
        out_specs=full_spec(len(outs)),
        scratch_shapes=list(scratch),
    )(*args)


def pack_body(lat_ref, pos_ref, cot_ref, fil_ref, zbuf_ref, lbuf_ref):
    natom = cot_ref.shape[0]
    nk = fil_ref.shape[0]
    width = cot_ref.shape[1]
    zbuf_ref[0:natom, :] = cot_ref[...]
    x = pos_ref[...]
    hi = x.astype(bf16).astype(f32)
    rest = x - hi
    mid = rest.astype(bf16).astype(f32)
    low = rest - mid
    zero = jnp.zeros_like(x)
    parts = jnp.concatenate([hi, mid, low, zero, zero, zero[:1]], 0).astype(bf16)
    for j in range(natom // width):
        zbuf_ref[natom + 16 * j : natom + 16 * (j + 1), :] = parts[:, j * width : (j + 1) * width]
    lbuf_ref[0:nk, :] = fil_ref[...]
    row = lax.broadcasted_iota(jnp.int32, (nk, width), 0)
    col = lax.broadcasted_iota(jnp.int32, (nk, width), 1)
    spread = (row == col % nk).astype(bf16)
    lat = lat_ref[...].astype(f32).astype(bf16)
    wide = jnp.dot(lat, spread, preferred_element_type=f32)
    lbuf_ref[nk : nk + 8, :] = jnp.concatenate([wide, wide, wide[:2]], 0)


def factor_body(nz, nq, natom, nk, *refs):
    zb = refs[:nz]
    lb = refs[nz : nz + nq]
    tile_ref, f_ref, fb_ref, acc_ref = refs[nz + nq :]
    width = zb[0].shape[1]
    per = width // nk
    nw = nq * nk
    lane = lax.broadcasted_iota(jnp.int32, (8, width), 1)
    cols = []
    for g in range(nq // per):
        piece = lb[g * per][nk : nk + 8, :]
        for j in range(1, per):
            piece = jnp.where(lane >= j * nk, lb[g * per + j][nk : nk + 8, :], piece)
        cols.append(piece)
    lat = jnp.concatenate(cols, 1)[:3]
    zero = jnp.zeros_like(lat)
    lat9 = jnp.concatenate([lat, lat, lat, zero, zero, zero[:1]], 0).astype(bf16)
    step = 32
    for z in range(nz):
        parts = jnp.concatenate(
            [zb[z][natom + 16 * j : natom + 16 * (j + 1), :] for j in range(natom // width)], 1
        )
        phase = lax.dot_general(parts, lat9, (((0,), (0,)), ((), ())), preferred_element_type=f32)
        for i in range(0, natom, step):
            c, s = cos_sin(phase[i : i + step])
            tile_ref[z * natom + i : z * natom + i + step, 0:nw] = c.astype(bf16)
            tile_ref[z * natom + i : z * natom + i + step, nw : 2 * nw] = s.astype(bf16)
        part = lax.dot_general(
            zb[z][0:natom, :],
            tile_ref[z * natom : (z + 1) * natom, :],
            (((0,), (0,)), ((), ())),
            preferred_element_type=f32,
        )
        if z == 0:
            acc_ref[...] = part
        else:
            acc_ref[...] += part
    total = acc_ref[...].T
    f_ref[...] = total
    fb_ref[...] = total.astype(bf16)


def shuffled(ref, flip, nq, nk):
    rows = [ref[h * nq * nk + (t ^ flip) * nk : h * nq * nk + ((t ^ flip) + 1) * nk, :] for h in range(2) for t in range(nq)]
    return jnp.concatenate(rows, 0).astype(f32)


def pair_body(nq, nk, own_ref, got_ref, f_ref, fb_ref):
    total = own_ref[...] + shuffled(got_ref, 1, nq, nk)
    f_ref[...] = total
    fb_ref[...] = total.astype(bf16)


def node_body(nz, nq, natom, nk, flips, scale, *refs):
    own_ref = refs[0]
    got = refs[1 : 1 + len(flips)]
    lb = refs[1 + len(flips) : 1 + len(flips) + nq]
    tile_ref, saved_ref = refs[1 + len(flips) + nq : 3 + len(flips) + nq]
    grad_ref = refs[3 + len(flips) + nq]
    outs = refs[4 + len(flips) + nq :]
    total = own_ref[...]
    for ref, flip in zip(got, flips):
        total = total + shuffled(ref, flip, nq, nk)
    total = total * scale
    nw = nq * nk
    fil = jnp.concatenate([lb[t][0:nk, :] for t in range(nq)], 0)
    weighted = jnp.concatenate([fil * total[:nw], fil * total[nw:]], 0).astype(bf16)
    grad_ref[...] = total[0:nk] * saved_ref[0] + total[nw : nw + nk] * saved_ref[1]
    for z in range(nz):
        part = jnp.dot(tile_ref[z * natom : (z + 1) * natom, :], weighted, preferred_element_type=f32)
        outs[z][...] = part.astype(outs[z].dtype)


def final_body(scale, *refs):
    total = refs[0][...]
    for ref in refs[1:-1]:
        total = total + ref[...].astype(f32)
    refs[-1][...] = (total * scale).astype(bf16)


def shape(dims, kind):
    return jax.ShapeDtypeStruct(dims, kind)


def local(lattice, positions, cotangent, filters, saved_factor):
    nz = lax.axis_size("atoms")
    nq = lax.axis_size("kvec")
    natom, width = cotangent.shape
    nk = lattice.shape[1]
    nw = nq * nk
    scale_n = 1.0 / math.sqrt(natom * nz * nq)
    scale_k = 1.0 / math.sqrt(nk * nz * nq)

    def swap(value, axis, size, flip):
        return lax.ppermute(value, axis, [(i, i ^ flip) for i in range(size)])

    zbuf, lbuf = call(
        pack_body,
        [shape((natom + 16 * (natom // width), width), bf16), shape((nk + 8, width), f32)],
        lattice,
        positions,
        cotangent,
        filters,
        keep_args=False,
    )
    zb = [zbuf] + [swap(zbuf, "atoms", nz, s) for s in range(1, nz)]
    lb = {0: lbuf}
    for s in range(2, nq, 2):
        lb[s] = swap(lbuf, "kvec", nq, s)
    for s in range(0, nq, 2):
        lb[s + 1] = swap(lb[s], "kvec", nq, 1)
    lb = [lb[s] for s in range(nq)]
    tile, part, part16 = call(
        lambda *refs: factor_body(nz, nq, natom, nk, *refs),
        [shape((nz * natom, 2 * nw), bf16), shape((2 * nw, width), f32), shape((2 * nw, width), bf16)],
        *zb,
        *lb,
        scratch=[pltpu.VMEM((width, 2 * nw), f32)],
    )
    pair, pair16 = call(
        lambda *refs: pair_body(nq, nk, *refs),
        [shape((2 * nw, width), f32), shape((2 * nw, width), bf16)],
        part,
        swap(part16, "kvec", nq, 1),
    )
    flips = list(range(2, nq, 2))
    got = [swap(pair16, "kvec", nq, s) for s in flips]
    filter_grad, *nodes = call(
        lambda *refs: node_body(nz, nq, natom, nk, flips, scale_n, *refs),
        [shape((nk, width), f32), shape((natom, width), f32)] + [shape((natom, width), bf16)] * (nz - 1),
        pair,
        *got,
        *lb,
        tile,
        saved_factor,
    )
    (node_grad,) = call(
        lambda *refs: final_body(scale_k, *refs),
        [shape((natom, width), bf16)],
        nodes[0],
        *[swap(nodes[s], "atoms", nz, s) for s in range(1, nz)],
        keep_outs=False,
    )
    return (node_grad, filter_grad)


def solution(mesh):
    in_specs = (
        P(None, ("atoms", "kvec")),
        P(None, ("beads", "atoms", "kvec")),
        P(("beads", "atoms", "kvec"), None),
        P(("atoms", "kvec"), None),
        P(None, ("beads", "atoms", "kvec"), None),
    )
    out_specs = (P(("beads", "atoms", "kvec"), None), P(("beads", "atoms", "kvec"), None))
    return jax.shard_map(local, mesh=mesh, in_specs=in_specs, out_specs=out_specs, check_vma=False)
```

```python
import math

import jax
import jax.numpy as jnp
from jax import lax
from jax.experimental import pallas as pl
from jax.experimental.pallas import tpu as pltpu
from jax.sharding import PartitionSpec as P

f32 = jnp.float32
bf16 = jnp.bfloat16


SIN_COEF = None
COS_COEF = None


def _fit():
    import numpy as np

    n = 4001
    t = np.cos(np.pi * (np.arange(n) + 0.5) / n)
    u = (t + 1.0) * 0.125
    r = np.sqrt(u)
    root = math.sqrt(2.0)
    sin_ratio = np.where(r > 1e-9, root * np.sin(np.pi * r) / np.maximum(r, 1e-9), root * np.pi)
    cheb = np.polynomial.chebyshev.Chebyshev
    s = cheb.fit(u, sin_ratio, 4, domain=[0.0, 0.25]).convert(kind=np.polynomial.Polynomial)
    c = cheb.fit(u, root * np.cos(np.pi * r), 4, domain=[0.0, 0.25]).convert(kind=np.polynomial.Polynomial)
    return tuple(float(v) for v in s.coef), tuple(float(v) for v in c.coef)


SIN_COEF, COS_COEF = _fit()


def _horner(coef, u):
    acc = jnp.full_like(u, coef[-1])
    for value in coef[-2::-1]:
        acc = acc * u + value
    return acc


def cos_sin(phase):
    r = phase - jnp.round(phase)
    u = r * r
    s = r * _horner(SIN_COEF, u)
    c = _horner(COS_COEF, u)
    return 1.0 - s * s, s * c


def full_spec(count):
    return [pl.BlockSpec(memory_space=pltpu.VMEM)] * count


VMEM_BUDGET = 4 * 1024 * 1024


def call(body, outs, *args, keep_args=True, keep_outs=True):
    if keep_args:
        args = [pltpu.with_memory_space_constraint(arg, pltpu.VMEM) for arg in args]
    if keep_outs:
        outs = [pltpu.VMEM(v.shape, v.dtype) for v in outs]
    return pl.pallas_call(
        body,
        out_shape=outs,
        in_specs=full_spec(len(args)),
        out_specs=full_spec(len(outs)),
    )(*args)


def pack_z_body(pos_ref, cot_ref, out_ref):
    natom, width = cot_ref.shape
    out_ref[0:natom, :] = cot_ref[...]
    x = pos_ref[...]
    hi = x.astype(bf16).astype(f32)
    rest = x - hi
    mid = rest.astype(bf16).astype(f32)
    low = rest - mid
    zero = jnp.zeros_like(x)
    parts = jnp.concatenate([hi, mid, low, zero, zero, zero[:1]], 0).astype(bf16)
    for j in range(natom // width):
        out_ref[natom + 16 * j : natom + 16 * (j + 1), :] = parts[:, j * width : (j + 1) * width]


def pack_k_body(lat_ref, fil_ref, out_ref):
    nk, width = fil_ref.shape
    out_ref[0:nk, :] = fil_ref[...]
    row = lax.broadcasted_iota(jnp.int32, (nk, width), 0)
    col = lax.broadcasted_iota(jnp.int32, (nk, width), 1)
    spread = (row == col % nk).astype(bf16)
    lat = lat_ref[...].astype(f32).astype(bf16)
    wide = jnp.dot(lat, spread, preferred_element_type=f32)
    out_ref[nk : nk + 8, :] = jnp.concatenate([wide, wide, wide[:2]], 0)


def factor_body(nq, natom, nk, first, last, *refs):
    zb = refs[0]
    lb = refs[1 : 1 + nq]
    rest = refs[1 + nq :]
    if not first:
        before_ref = rest[0]
        rest = rest[1:]
    tile_ref = rest[0]
    width = zb.shape[1]
    per = width // nk
    nw = nq * nk
    lane = lax.broadcasted_iota(jnp.int32, (8, width), 1)
    cols = []
    for g in range(nq // per):
        piece = lb[g * per][nk : nk + 8, :]
        for j in range(1, per):
            piece = jnp.where(lane >= j * nk, lb[g * per + j][nk : nk + 8, :], piece)
        cols.append(piece)
    lat = jnp.concatenate(cols, 1)[:3]
    zero = jnp.zeros_like(lat)
    lat9 = jnp.concatenate([lat, lat, lat, zero, zero, zero[:1]], 0).astype(bf16)
    parts = jnp.concatenate([zb[natom + 16 * j : natom + 16 * (j + 1), :] for j in range(natom // width)], 1)
    phase = lax.dot_general(parts, lat9, (((0,), (0,)), ((), ())), preferred_element_type=f32)
    step = 32
    for i in range(0, natom, step):
        c, s = cos_sin(phase[i : i + step])
        tile_ref[i : i + step, 0:nw] = c.astype(bf16)
        tile_ref[i : i + step, nw : 2 * nw] = s.astype(bf16)
    total = lax.dot_general(zb[0:natom, :], tile_ref[...], (((0,), (0,)), ((), ())), preferred_element_type=f32)
    if not first:
        total = total + before_ref[...]
    if last:
        total = total.T
        rest[2][...] = total.astype(bf16)
    rest[1][...] = total


def shuffled(ref, flip, nq, nk):
    rows = [ref[h * nq * nk + (t ^ flip) * nk : h * nq * nk + ((t ^ flip) + 1) * nk, :] for h in range(2) for t in range(nq)]
    return jnp.concatenate(rows, 0).astype(f32)


def pair_body(nq, nk, own_ref, got_ref, f_ref, fb_ref):
    total = own_ref[...] + shuffled(got_ref, 1, nq, nk)
    f_ref[...] = total
    fb_ref[...] = total.astype(bf16)


def weight_body(nq, nk, flips, scale, *refs):
    own_ref = refs[0]
    got = refs[1 : 1 + len(flips)]
    lb = refs[1 + len(flips) : 1 + len(flips) + nq]
    tile_ref, weight_ref, head_ref, node_ref = refs[1 + len(flips) + nq :]
    total = own_ref[...]
    for ref, flip in zip(got, flips):
        total = total + shuffled(ref, flip, nq, nk)
    total = total * scale
    nw = nq * nk
    fil = jnp.concatenate([lb[t][0:nk, :] for t in range(nq)], 0)
    weighted = jnp.concatenate([fil * total[:nw], fil * total[nw:]], 0).astype(bf16)
    weight_ref[...] = weighted
    head_ref[...] = jnp.concatenate([total[0:nk], total[nw : nw + nk]], 0)
    node_ref[...] = jnp.dot(tile_ref[...], weighted, preferred_element_type=f32).astype(node_ref.dtype)


def node_body(tile_ref, weight_ref, node_ref):
    node_ref[...] = jnp.dot(tile_ref[...], weight_ref[...], preferred_element_type=f32).astype(node_ref.dtype)


def own_body(tile_ref, weight_ref, head_ref, saved_ref, node_ref, grad_ref):
    node_body(tile_ref, weight_ref, node_ref)
    nk = grad_ref.shape[0]
    grad_ref[...] = head_ref[0:nk] * saved_ref[0] + head_ref[nk : 2 * nk] * saved_ref[1]


def final_body(scale, *refs):
    total = refs[0][...]
    for ref in refs[1:-1]:
        total = total + ref[...].astype(f32)
    refs[-1][...] = (total * scale).astype(bf16)


def shape(dims, kind):
    return jax.ShapeDtypeStruct(dims, kind)


def local(lattice, positions, cotangent, filters, saved_factor):
    nz = lax.axis_size("atoms")
    nq = lax.axis_size("kvec")
    natom, width = cotangent.shape
    nk = lattice.shape[1]
    nw = nq * nk
    scale_n = 1.0 / math.sqrt(natom * nz * nq)
    scale_k = 1.0 / math.sqrt(nk * nz * nq)
    keep = nz * natom * 2 * nw * 2 <= VMEM_BUDGET

    def swap(value, axis, size, flip):
        return lax.ppermute(value, axis, [(i, i ^ flip) for i in range(size)])

    (zbuf,) = call(
        pack_z_body,
        [shape((natom + 16 * (natom // width), width), bf16)],
        positions,
        cotangent,
        keep_args=False,
        keep_outs=keep,
    )
    (lbuf,) = call(pack_k_body, [shape((nk + 8, width), f32)], lattice, filters, keep_args=False, keep_outs=keep)
    far = list(range(nz - 1, 0, -1))
    zb = {0: zbuf}
    for s in far:
        zb[s] = swap(zbuf, "atoms", nz, s)
    lb = {0: lbuf}
    for s in range(2, nq, 2):
        lb[s] = swap(lbuf, "kvec", nq, s)
    for s in range(0, nq, 2):
        lb[s + 1] = swap(lb[s], "kvec", nq, 1)
    lb = [lb[s] for s in range(nq)]
    tiles = {}
    total = None
    order = [0] + far
    for s in order:
        first, last = s == order[0], s == order[-1]
        dims = (2 * nw, width) if last else (width, 2 * nw)
        outs = [shape((natom, 2 * nw), bf16), shape(dims, f32)] + ([shape(dims, bf16)] if last else [])
        body = lambda *refs, first=first, last=last: factor_body(nq, natom, nk, first, last, *refs)
        tiles[s], total, *sent = call(body, outs, zb[s], *lb, *([] if first else [total]), keep_args=keep, keep_outs=keep)
    pair, pair16 = call(
        lambda *refs: pair_body(nq, nk, *refs),
        [shape((2 * nw, width), f32), shape((2 * nw, width), bf16)],
        total,
        swap(sent[0], "kvec", nq, 1),
        keep_args=keep,
        keep_outs=keep,
    )
    flips = list(range(2, nq, 2))
    got = [swap(pair16, "kvec", nq, s) for s in flips]
    far = far or [0]
    weighted, head, node = call(
        lambda *refs: weight_body(nq, nk, flips, scale_n, *refs),
        [shape((2 * nw, width), bf16), shape((2 * nk, width), f32), shape((natom, width), bf16)],
        pair,
        *got,
        *lb,
        tiles[far[0]],
        keep_args=keep,
        keep_outs=keep,
    )
    landed = [swap(node, "atoms", nz, far[0])] if nz > 1 else []
    for s in far[1:]:
        (node,) = call(node_body, [shape((natom, width), bf16)], tiles[s], weighted, keep_args=keep, keep_outs=keep)
        landed.append(swap(node, "atoms", nz, s))
    own, filter_grad = call(
        own_body,
        [shape((natom, width), f32), shape((nk, width), f32)],
        tiles[0],
        weighted,
        head,
        saved_factor,
        keep_args=keep,
        keep_outs=keep,
    )
    (node_grad,) = call(
        lambda *refs: final_body(scale_k, *refs),
        [shape((natom, width), bf16)],
        own,
        *landed,
        keep_args=keep,
        keep_outs=False,
    )
    return (node_grad, filter_grad)


def solution(mesh):
    in_specs = (
        P(None, ("atoms", "kvec")),
        P(None, ("beads", "atoms", "kvec")),
        P(("beads", "atoms", "kvec"), None),
        P(("atoms", "kvec"), None),
        P(None, ("beads", "atoms", "kvec"), None),
    )
    out_specs = (P(("beads", "atoms", "kvec"), None), P(("beads", "atoms", "kvec"), None))
    return jax.shard_map(local, mesh=mesh, in_specs=in_specs, out_specs=out_specs, check_vma=False)
```

```python
import math

import jax
import jax.numpy as jnp
from jax import lax
from jax.experimental import pallas as pl
from jax.experimental.pallas import tpu as pltpu
from jax.sharding import PartitionSpec as P


f32 = jnp.float32
bf16 = jnp.bfloat16


SIN_COEF = None
COS_COEF = None


def _fit():
    import numpy as np

    n = 4001
    t = np.cos(np.pi * (np.arange(n) + 0.5) / n)
    u = (t + 1.0) * 0.125
    r = np.sqrt(u)
    root = math.sqrt(2.0)
    sin_ratio = np.where(r > 1e-9, root * np.sin(np.pi * r) / np.maximum(r, 1e-9), root * np.pi)
    cheb = np.polynomial.chebyshev.Chebyshev
    s = cheb.fit(u, sin_ratio, 4, domain=[0.0, 0.25]).convert(kind=np.polynomial.Polynomial)
    c = cheb.fit(u, root * np.cos(np.pi * r), 4, domain=[0.0, 0.25]).convert(kind=np.polynomial.Polynomial)
    return tuple(float(v) for v in s.coef), tuple(float(v) for v in c.coef)


SIN_COEF, COS_COEF = _fit()


def _horner(coef, u):
    acc = jnp.full_like(u, coef[-1])
    for value in coef[-2::-1]:
        acc = acc * u + value
    return acc


def cos_sin(phase):
    r = phase - jnp.round(phase)
    u = r * r
    s = r * _horner(SIN_COEF, u)
    c = _horner(COS_COEF, u)
    return 1.0 - s * s, s * c


def full_spec(count):
    return [pl.BlockSpec(memory_space=pltpu.VMEM)] * count


VMEM_BUDGET = 4 * 1024 * 1024


def call(body, outs, *args, keep_args=True, keep_outs=True):
    if keep_args:
        args = [pltpu.with_memory_space_constraint(arg, pltpu.VMEM) for arg in args]
    if keep_outs:
        outs = [pltpu.VMEM(v.shape, v.dtype) for v in outs]
    return pl.pallas_call(
        body,
        out_shape=outs,
        in_specs=full_spec(len(args)),
        out_specs=full_spec(len(outs)),
    )(*args)


def pack_body(lat_ref, pos_ref, cot_ref, out_ref, wide_ref):
    natom, width = cot_ref.shape
    nk = lat_ref.shape[1]
    out_ref[0:natom, :] = cot_ref[...]
    x = pos_ref[...]
    hi = x.astype(bf16).astype(f32)
    rest = x - hi
    mid = rest.astype(bf16).astype(f32)
    low = rest - mid
    zero = jnp.zeros_like(x)
    parts = jnp.concatenate([hi, mid, low, zero, zero, zero[:1]], 0).astype(bf16)
    for j in range(natom // width):
        out_ref[natom + 16 * j : natom + 16 * (j + 1), :] = parts[:, j * width : (j + 1) * width]
    row = lax.broadcasted_iota(jnp.int32, (nk, width), 0)
    col = lax.broadcasted_iota(jnp.int32, (nk, width), 1)
    spread = (row == col % nk).astype(bf16)
    lat = lat_ref[...].astype(f32).astype(bf16)
    wide = jnp.dot(lat, spread, preferred_element_type=f32)
    wide_ref[...] = jnp.concatenate([wide, wide, wide[:2]], 0)


def join_body(own_ref, got_ref, out_ref):
    out_ref[0:8, :] = own_ref[...]
    out_ref[8:16, :] = got_ref[...]


def table_body(nk, lat_ref, out_ref):
    width = lat_ref.shape[1]
    zero = jnp.zeros((3, width), f32)
    for h in range(2):
        lat = lat_ref[8 * h : 8 * h + 3, :]
        cols = jnp.concatenate([lat, lat, lat, zero, zero, zero[:1]], 0).T
        out_ref[h * nk : (h + 1) * nk, :] = cols[0:nk].astype(bf16)


def factor_body(natom, nk, blocks, first, last, *refs):
    zb = refs[0]
    refs = refs[1:]
    count = len(blocks)
    tables, refs = refs[:count], refs[count:]
    before, refs = ((), refs) if first else (refs[:count], refs[count:])
    tiles, outs = refs[:count], refs[count:]
    width = zb.shape[1]
    parts = jnp.concatenate([zb[natom + 16 * j : natom + 16 * (j + 1), :] for j in range(natom // width)], 1)
    phases = [
        jnp.dot(table[h * nk : (h + 1) * nk, :], parts, preferred_element_type=f32)
        for table, h in zip(tables, (t % 2 for t in blocks))
    ]
    cot = zb[0:natom, :]
    step = 32
    for b in range(count):
        for i in range(0, nk, step):
            for k, value in enumerate(cos_sin(phases[b][i : i + step])):
                rows = pl.ds(k * nk + i, step)
                value = value.astype(bf16)
                tiles[b][rows, :] = value
                total = jnp.dot(value, cot, preferred_element_type=f32)
                if not first:
                    total = total + before[b][rows, :]
                if last:
                    rows = pl.ds(2 * nk * b + k * nk + i, step)
                    outs[0][rows, :] = total.astype(outs[0].dtype)
                else:
                    outs[b][rows, :] = total


def shuffled(ref, flip, half, nk):
    rows = [ref[2 * nk * (t ^ flip) : 2 * nk * ((t ^ flip) + 1), :] for t in range(half)]
    return jnp.concatenate(rows, 0).astype(f32)


def pair_body(own_ref, got_ref, f_ref, fb_ref):
    total = own_ref[...] + got_ref[...].astype(f32)
    f_ref[...] = total
    fb_ref[...] = total.astype(bf16)


def weight_body(half, nk, flips, scale, *refs):
    total = refs[0][...]
    for ref, flip in zip(refs[1:], flips):
        total = total + shuffled(ref, flip // 2, half, nk)
    total = total * scale
    fb = refs[1 + len(flips) : 1 + len(flips) + half]
    weight_ref, head_ref = refs[1 + len(flips) + half :]
    for t in range(half):
        fil = fb[t][...]
        rows = total[2 * nk * t : 2 * nk * (t + 1)] * jnp.concatenate([fil, fil], 0)
        weight_ref[:, 2 * nk * t : 2 * nk * (t + 1)] = rows.T.astype(bf16)
    head_ref[...] = total[0 : 2 * nk]


def part_of(weight_ref, tiles):
    tile = jnp.concatenate([ref[...] for ref in tiles], 0)
    return jnp.dot(weight_ref[...], tile, preferred_element_type=f32)


def mine_body(nz, half, weight_ref, *refs):
    for z in range(nz):
        refs[nz * half + z][...] = part_of(weight_ref, refs[z * half : (z + 1) * half])


def node_body(half, part_ref, weight_ref, *refs):
    total = part_ref[...] + part_of(weight_ref, refs[:half])
    refs[half][...] = total.T.astype(refs[half].dtype)


def own_body(half, head_ref, saved_ref, part_ref, weight_ref, *refs):
    node_body(half, part_ref, weight_ref, *refs)
    grad_ref = refs[half + 1]
    nk = grad_ref.shape[0]
    grad_ref[...] = head_ref[0:nk] * saved_ref[0] + head_ref[nk : 2 * nk] * saved_ref[1]


def final_body(scale, *refs):
    total = refs[0][...]
    for ref in refs[1:-1]:
        total = total + ref[...].astype(f32)
    refs[-1][...] = (total * scale).astype(bf16)


def shape(dims, kind):
    return jax.ShapeDtypeStruct(dims, kind)


def local(lattice, positions, cotangent, filters, saved_factor):
    nz = lax.axis_size("atoms")
    nq = lax.axis_size("kvec")
    natom, width = cotangent.shape
    nk = lattice.shape[1]
    half = nq // 2
    count = half * nk
    scale_n = 1.0 / math.sqrt(natom * nz * nq)
    scale_k = 1.0 / math.sqrt(nk * nz * nq)
    keep = nz * natom * 4 * count * 2 <= VMEM_BUDGET

    def swap(value, axis, size, flip):
        return lax.ppermute(value, axis, [(i, i ^ flip) for i in range(size)])

    def run(body, outs, *args, keep_args=keep, keep_outs=keep):
        return call(body, outs, *args, keep_args=keep_args, keep_outs=keep_outs)

    zbuf, wide = run(
        pack_body,
        [shape((natom + 16 * (natom // width), width), bf16), shape((8, width), f32)],
        lattice,
        positions,
        cotangent,
        keep_args=False,
    )
    far = list(range(nz - 1, 0, -1))
    flips = list(range(2, nq, 2))
    zb = {0: zbuf}
    for s in far:
        zb[s] = swap(zbuf, "atoms", nz, s)
    (cores,) = run(join_body, [shape((16, width), f32)], wide, swap(wide, "kvec", nq, 1))
    lats = [cores] + [swap(cores, "kvec", nq, s) for s in flips]
    fils = [filters] + [swap(filters, "kvec", nq, s) for s in flips]
    table = {}
    for s, lat in zip([0] + flips, lats):
        (both,) = run(lambda *refs: table_body(nk, *refs), [shape((2 * nk, 16), bf16)], lat)
        table[s] = table[s + 1] = both
    mine = list(range(0, nq, 2))
    theirs = list(range(1, nq, 2))
    tiles = {}
    total = {}

    def factor(s, blocks, first=False, last=None):
        outs = [shape((2 * nk, natom), bf16)] * len(blocks)
        sums = [shape((2 * nk, width), f32)] * len(blocks)
        if last is not None:
            sums = [shape((2 * nk * len(blocks), width), last)]
        args = [zb[s]] + [table[t] for t in blocks] + ([] if first else [total[t] for t in blocks])
        body = lambda *refs: factor_body(natom, nk, blocks, first, last is not None, *refs)
        got = run(body, outs + sums, *args)
        for t, tile in zip(blocks, got):
            tiles[s, t] = tile
        if last is not None:
            return got[-1]
        for t, value in zip(blocks, got[len(blocks) :]):
            total[t] = value
        return None

    order = [0] + far
    for s in order[:-1]:
        for t in range(0, nq, 2):
            factor(s, [t, t + 1], first=s == order[0])
    sent = factor(order[-1], theirs, last=bf16)
    kept = factor(order[-1], mine, last=f32)
    pair, pair16 = run(
        pair_body,
        [shape((2 * count, width), f32), shape((2 * count, width), bf16)],
        kept,
        swap(sent, "kvec", nq, 1),
    )
    got = [swap(pair16, "kvec", nq, s) for s in flips]
    weight, head = run(
        lambda *refs: weight_body(half, nk, flips, scale_n, *refs),
        [shape((width, 2 * count), bf16), shape((2 * nk, width), f32)],
        pair,
        *got,
        *fils,
    )
    other = swap(weight, "kvec", nq, 1)
    parts = run(
        lambda *refs: mine_body(nz, half, *refs),
        [shape((width, natom), f32)] * nz,
        weight,
        *[tiles[s, t] for s in order for t in mine],
    )
    landed = []
    for s, part in zip(order[1:], parts[1:]):
        (node,) = run(
            lambda *refs: node_body(half, *refs),
            [shape((natom, width), bf16)],
            part,
            other,
            *[tiles[s, t] for t in theirs],
        )
        landed.append(swap(node, "atoms", nz, s))
    own, filter_grad = run(
        lambda *refs: own_body(half, *refs),
        [shape((natom, width), f32), shape((nk, width), f32)],
        head,
        saved_factor,
        parts[0],
        other,
        *[tiles[0, t] for t in theirs],
    )
    (node_grad,) = run(
        lambda *refs: final_body(scale_k, *refs),
        [shape((natom, width), bf16)],
        own,
        *landed,
        keep_outs=False,
    )
    return (node_grad, filter_grad)


def solution(mesh):
    in_specs = (
        P(None, ("atoms", "kvec")),
        P(None, ("beads", "atoms", "kvec")),
        P(("beads", "atoms", "kvec"), None),
        P(("atoms", "kvec"), None),
        P(None, ("beads", "atoms", "kvec"), None),
    )
    out_specs = (P(("beads", "atoms", "kvec"), None), P(("beads", "atoms", "kvec"), None))
    return jax.shard_map(local, mesh=mesh, in_specs=in_specs, out_specs=out_specs, check_vma=False)
```

```python
import math

import jax
import jax.numpy as jnp
from jax import lax
from jax.experimental import pallas as pl
from jax.experimental.pallas import tpu as pltpu
from jax.sharding import PartitionSpec as P


f32 = jnp.float32
bf16 = jnp.bfloat16


SIN_COEF = None
COS_COEF = None


def _fit():
    import numpy as np

    n = 4001
    t = np.cos(np.pi * (np.arange(n) + 0.5) / n)
    u = (t + 1.0) * 0.125
    r = np.sqrt(u)
    root = math.sqrt(2.0)
    sin_ratio = np.where(r > 1e-9, root * np.sin(np.pi * r) / np.maximum(r, 1e-9), root * np.pi)
    cheb = np.polynomial.chebyshev.Chebyshev
    s = cheb.fit(u, sin_ratio, 4, domain=[0.0, 0.25]).convert(kind=np.polynomial.Polynomial)
    c = cheb.fit(u, root * np.cos(np.pi * r), 4, domain=[0.0, 0.25]).convert(kind=np.polynomial.Polynomial)
    return tuple(float(v) for v in s.coef), tuple(float(v) for v in c.coef)


SIN_COEF, COS_COEF = _fit()


def _horner(coef, u):
    acc = jnp.full_like(u, coef[-1])
    for value in coef[-2::-1]:
        acc = acc * u + value
    return acc


def cos_sin(phase):
    r = phase - jnp.round(phase)
    u = r * r
    s = r * _horner(SIN_COEF, u)
    c = _horner(COS_COEF, u)
    return 1.0 - s * s, s * c


def full_spec(count):
    return [pl.BlockSpec(memory_space=pltpu.VMEM)] * count


VMEM_BUDGET = 4 * 1024 * 1024


def call(body, outs, *args, keep_args=True, keep_outs=True):
    if keep_args:
        args = [pltpu.with_memory_space_constraint(arg, pltpu.VMEM) for arg in args]
    if keep_outs:
        outs = [pltpu.VMEM(v.shape, v.dtype) for v in outs]
    return pl.pallas_call(
        body,
        out_shape=outs,
        in_specs=full_spec(len(args)),
        out_specs=full_spec(len(outs)),
    )(*args)


def pack_body(lat_ref, pos_ref, cot_ref, out_ref, wide_ref):
    natom, width = cot_ref.shape
    nk = lat_ref.shape[1]
    out_ref[0:natom, :] = cot_ref[...]
    x = pos_ref[...]
    hi = x.astype(bf16).astype(f32)
    rest = x - hi
    mid = rest.astype(bf16).astype(f32)
    low = rest - mid
    zero = jnp.zeros_like(x)
    parts = jnp.concatenate([hi, mid, low, zero, zero, zero[:1]], 0).astype(bf16)
    for j in range(natom // width):
        out_ref[natom + 16 * j : natom + 16 * (j + 1), :] = parts[:, j * width : (j + 1) * width]
    row = lax.broadcasted_iota(jnp.int32, (nk, width), 0)
    col = lax.broadcasted_iota(jnp.int32, (nk, width), 1)
    spread = (row == col % nk).astype(bf16)
    lat = lat_ref[...].astype(f32).astype(bf16)
    wide = jnp.dot(lat, spread, preferred_element_type=f32)
    wide_ref[...] = jnp.concatenate([wide, wide, wide[:2]], 0)


def join_body(own_ref, got_ref, out_ref):
    out_ref[0:8, :] = own_ref[...]
    out_ref[8:16, :] = got_ref[...]


def table_body(nk, lat_ref, out_ref):
    width = lat_ref.shape[1]
    zero = jnp.zeros((3, width), f32)
    for h in range(2):
        lat = lat_ref[8 * h : 8 * h + 3, :]
        cols = jnp.concatenate([lat, lat, lat, zero, zero, zero[:1]], 0).T
        out_ref[h * nk : (h + 1) * nk, :] = cols[0:nk].astype(bf16)


def factor_body(natom, nk, pairs, blocks, started, last, *refs):
    atoms = sorted({z for z, t in pairs})
    zb, refs = dict(zip(atoms, refs)), refs[len(atoms) :]
    tables, refs = dict(zip(blocks, refs)), refs[len(blocks) :]
    before, refs = (dict(zip(blocks, refs)), refs[len(blocks) :]) if started else ({}, refs)
    tiles, outs = dict(zip(pairs, refs)), refs[len(pairs) :]
    width = zb[atoms[0]].shape[1]
    parts = {
        z: jnp.concatenate([ref[natom + 16 * j : natom + 16 * (j + 1), :] for j in range(natom // width)], 1)
        for z, ref in zb.items()
    }
    phases = {}
    for z, t in pairs:
        table = tables[t][(t % 2) * nk : (t % 2 + 1) * nk, :]
        phases[z, t] = jnp.dot(table, parts[z], preferred_element_type=f32)
    cot = {z: ref[0:natom, :] for z, ref in zb.items()}
    step = 32
    for b, t in enumerate(blocks):
        for i in range(0, nk, step):
            sums = [None, None]
            for z in atoms:
                for k, value in enumerate(cos_sin(phases[z, t][i : i + step])):
                    value = value.astype(bf16)
                    tiles[z, t][k * nk + i : k * nk + i + step, :] = value
                    part = jnp.dot(value, cot[z], preferred_element_type=f32)
                    sums[k] = part if sums[k] is None else sums[k] + part
            for k, total in enumerate(sums):
                row = k * nk + i
                if started:
                    total = total + before[t][row : row + step, :]
                if last:
                    outs[0][2 * nk * b + row : 2 * nk * b + row + step, :] = total.astype(outs[0].dtype)
                else:
                    outs[b][row : row + step, :] = total


def shuffled(ref, flip, half, nk):
    rows = [ref[2 * nk * (t ^ flip) : 2 * nk * ((t ^ flip) + 1), :] for t in range(half)]
    return jnp.concatenate(rows, 0).astype(f32)


def pair_body(own_ref, got_ref, f_ref, fb_ref):
    total = own_ref[...] + got_ref[...].astype(f32)
    f_ref[...] = total
    fb_ref[...] = total.astype(bf16)


def weight_body(half, nk, flips, scale, *refs):
    total = refs[0][...]
    for ref, flip in zip(refs[1:], flips):
        total = total + shuffled(ref, flip // 2, half, nk)
    total = total * scale
    fb = refs[1 + len(flips) : 1 + len(flips) + half]
    weight_ref, head_ref = refs[1 + len(flips) + half :]
    for t in range(half):
        fil = fb[t][...]
        rows = total[2 * nk * t : 2 * nk * (t + 1)] * jnp.concatenate([fil, fil], 0)
        weight_ref[:, 2 * nk * t : 2 * nk * (t + 1)] = rows.T.astype(bf16)
    head_ref[...] = total[0 : 2 * nk]


def part_of(weight_ref, tiles):
    tile = jnp.concatenate([ref[...] for ref in tiles], 0)
    return jnp.dot(weight_ref[...], tile, preferred_element_type=f32)


def mine_body(nz, half, weight_ref, *refs):
    for z in range(nz):
        refs[nz * half + z][...] = part_of(weight_ref, refs[z * half : (z + 1) * half])


def node_body(half, part_ref, weight_ref, *refs):
    total = part_ref[...] + part_of(weight_ref, refs[:half])
    refs[half][...] = total.T.astype(refs[half].dtype)


def own_body(half, head_ref, saved_ref, part_ref, weight_ref, *refs):
    node_body(half, part_ref, weight_ref, *refs)
    grad_ref = refs[half + 1]
    nk = grad_ref.shape[0]
    grad_ref[...] = head_ref[0:nk] * saved_ref[0] + head_ref[nk : 2 * nk] * saved_ref[1]


def final_body(scale, *refs):
    total = refs[0][...]
    for ref in refs[1:-1]:
        total = total + ref[...].astype(f32)
    refs[-1][...] = (total * scale).astype(bf16)


def shape(dims, kind):
    return jax.ShapeDtypeStruct(dims, kind)


def local(lattice, positions, cotangent, filters, saved_factor):
    nz = lax.axis_size("atoms")
    nq = lax.axis_size("kvec")
    natom, width = cotangent.shape
    nk = lattice.shape[1]
    half = nq // 2
    count = half * nk
    scale_n = 1.0 / math.sqrt(natom * nz * nq)
    scale_k = 1.0 / math.sqrt(nk * nz * nq)
    keep = nz * natom * 4 * count * 2 <= VMEM_BUDGET

    def swap(value, axis, size, flip):
        return lax.ppermute(value, axis, [(i, i ^ flip) for i in range(size)])

    def run(body, outs, *args, keep_args=keep, keep_outs=keep):
        return call(body, outs, *args, keep_args=keep_args, keep_outs=keep_outs)

    zbuf, wide = run(
        pack_body,
        [shape((natom + 16 * (natom // width), width), bf16), shape((8, width), f32)],
        lattice,
        positions,
        cotangent,
        keep_args=False,
    )
    far = list(range(nz - 1, 0, -1))
    flips = list(range(2, nq, 2))
    zb = {0: zbuf}
    for s in far:
        zb[s] = swap(zbuf, "atoms", nz, s)
    (cores,) = run(join_body, [shape((16, width), f32)], wide, swap(wide, "kvec", nq, 1))
    lats = [cores] + [swap(cores, "kvec", nq, s) for s in flips]
    fils = [filters] + [swap(filters, "kvec", nq, s) for s in flips]
    table = {}
    for s, lat in zip([0] + flips, lats):
        (both,) = run(lambda *refs: table_body(nk, *refs), [shape((2 * nk, 16), bf16)], lat)
        table[s] = table[s + 1] = both
    mine = list(range(0, nq, 2))
    theirs = list(range(1, nq, 2))
    tiles = {}
    total = {}

    def factor(atoms, blocks, last=None):
        pairs = [(z, t) for z in sorted(atoms) for t in blocks]
        outs = [shape((2 * nk, natom), bf16)] * len(pairs)
        if last is None:
            outs += [shape((2 * nk, width), f32)] * len(blocks)
        else:
            outs.append(shape((2 * nk * len(blocks), width), last))
        started = blocks[0] in total
        args = [zb[z] for z in sorted(atoms)] + [table[t] for t in blocks] + [total[t] for t in blocks if started]
        body = lambda *refs: factor_body(natom, nk, pairs, blocks, started, last is not None, *refs)
        got = run(body, outs, *args)
        tiles.update(zip(pairs, got))
        if last is None:
            total.update(zip(blocks, got[len(pairs) :]))
        return got[-1]

    order = [0] + far
    early = order[: min(2, len(order) - 1)]
    for z in early:
        factor([z], [0, 1])
    for t in flips:
        factor(early, [t, t + 1])
    for z in order[len(early) : -1]:
        factor([z], list(range(nq)))
    sent = factor(order[-1:], theirs, bf16)
    kept = factor(order[-1:], mine, f32)
    pair, pair16 = run(
        pair_body, [shape((2 * count, width), f32), shape((2 * count, width), bf16)], kept, swap(sent, "kvec", nq, 1)
    )
    got = [swap(pair16, "kvec", nq, s) for s in flips]
    weight, head = run(
        lambda *refs: weight_body(half, nk, flips, scale_n, *refs),
        [shape((width, 2 * count), bf16), shape((2 * nk, width), f32)],
        pair,
        *got,
        *fils,
    )
    other = swap(weight, "kvec", nq, 1)
    parts = run(
        lambda *refs: mine_body(nz, half, *refs),
        [shape((width, natom), f32)] * nz,
        weight,
        *[tiles[s, t] for s in order for t in mine],
    )
    landed = []
    for s, part in zip(order[1:], parts[1:]):
        (node,) = run(
            lambda *refs: node_body(half, *refs),
            [shape((natom, width), bf16)],
            part,
            other,
            *[tiles[s, t] for t in theirs],
        )
        landed.append(swap(node, "atoms", nz, s))
    own, filter_grad = run(
        lambda *refs: own_body(half, *refs),
        [shape((natom, width), f32), shape((nk, width), f32)],
        head,
        saved_factor,
        parts[0],
        other,
        *[tiles[0, t] for t in theirs],
    )
    (node_grad,) = run(
        lambda *refs: final_body(scale_k, *refs), [shape((natom, width), bf16)], own, *landed, keep_outs=False
    )
    return (node_grad, filter_grad)


def solution(mesh):
    in_specs = (
        P(None, ("atoms", "kvec")),
        P(None, ("beads", "atoms", "kvec")),
        P(("beads", "atoms", "kvec"), None),
        P(("atoms", "kvec"), None),
        P(None, ("beads", "atoms", "kvec"), None),
    )
    out_specs = (P(("beads", "atoms", "kvec"), None), P(("beads", "atoms", "kvec"), None))
    return jax.shard_map(local, mesh=mesh, in_specs=in_specs, out_specs=out_specs, check_vma=False)
```

```python
import math

import jax
import jax.numpy as jnp
from jax import lax
from jax.experimental import pallas as pl
from jax.experimental.pallas import tpu as pltpu
from jax.sharding import PartitionSpec as P


f32 = jnp.float32
bf16 = jnp.bfloat16


SIN_COEF = None
COS_COEF = None


def _fit():
    import numpy as np

    n = 4001
    t = np.cos(np.pi * (np.arange(n) + 0.5) / n)
    u = (t + 1.0) * 0.125
    r = np.sqrt(u)
    root = math.sqrt(2.0)
    sin_ratio = np.where(r > 1e-9, root * np.sin(np.pi * r) / np.maximum(r, 1e-9), root * np.pi)
    cheb = np.polynomial.chebyshev.Chebyshev
    s = cheb.fit(u, sin_ratio, 4, domain=[0.0, 0.25]).convert(kind=np.polynomial.Polynomial)
    c = cheb.fit(u, root * np.cos(np.pi * r), 4, domain=[0.0, 0.25]).convert(kind=np.polynomial.Polynomial)
    return tuple(float(v) for v in s.coef), tuple(float(v) for v in c.coef)


SIN_COEF, COS_COEF = _fit()


def _horner(coef, u):
    acc = jnp.full_like(u, coef[-1])
    for value in coef[-2::-1]:
        acc = acc * u + value
    return acc


def cos_sin(phase):
    r = phase - jnp.round(phase)
    u = r * r
    s = r * _horner(SIN_COEF, u)
    c = _horner(COS_COEF, u)
    return 1.0 - s * s, s * c


def full_spec(count):
    return [pl.BlockSpec(memory_space=pltpu.VMEM)] * count


VMEM_BUDGET = 4 * 1024 * 1024


def call(body, outs, *args, keep_args=True, keep_outs=True):
    if keep_args:
        args = [pltpu.with_memory_space_constraint(arg, pltpu.VMEM) for arg in args]
    if keep_outs:
        outs = [pltpu.VMEM(v.shape, v.dtype) for v in outs]
    return pl.pallas_call(
        body,
        out_shape=outs,
        in_specs=full_spec(len(args)),
        out_specs=full_spec(len(outs)),
    )(*args)


def pack_body(lat_ref, pos_ref, cot_ref, out_ref, wide_ref):
    natom, width = cot_ref.shape
    nk = lat_ref.shape[1]
    out_ref[0:natom, :] = cot_ref[...]
    x = pos_ref[...]
    hi = x.astype(bf16).astype(f32)
    rest = x - hi
    mid = rest.astype(bf16).astype(f32)
    low = rest - mid
    zero = jnp.zeros_like(x)
    parts = jnp.concatenate([hi, mid, low, zero, zero, zero[:1]], 0).astype(bf16)
    for j in range(natom // width):
        out_ref[natom + 16 * j : natom + 16 * (j + 1), :] = parts[:, j * width : (j + 1) * width]
    row = lax.broadcasted_iota(jnp.int32, (nk, width), 0)
    col = lax.broadcasted_iota(jnp.int32, (nk, width), 1)
    spread = (row == col % nk).astype(bf16)
    lat = lat_ref[...].astype(f32).astype(bf16)
    wide = jnp.dot(lat, spread, preferred_element_type=f32)
    wide_ref[...] = jnp.concatenate([wide, wide, wide[:2]], 0)


def join_body(own_ref, got_ref, out_ref):
    out_ref[0:8, :] = own_ref[...]
    out_ref[8:16, :] = got_ref[...]


def table_body(nk, lat_ref, out_ref):
    width = lat_ref.shape[1]
    zero = jnp.zeros((3, width), f32)
    for h in range(2):
        lat = lat_ref[8 * h : 8 * h + 3, :]
        cols = jnp.concatenate([lat, lat, lat, zero, zero, zero[:1]], 0).T
        out_ref[h * nk : (h + 1) * nk, :] = cols[0:nk].astype(bf16)


def factor_body(natom, nk, pairs, blocks, started, last, *refs):
    atoms = sorted({z for z, t in pairs})
    zb, refs = dict(zip(atoms, refs)), refs[len(atoms) :]
    tables, refs = dict(zip(blocks, refs)), refs[len(blocks) :]
    before, refs = (dict(zip(blocks, refs)), refs[len(blocks) :]) if started else ({}, refs)
    tiles, outs = dict(zip(pairs, refs)), refs[len(pairs) :]
    width = zb[atoms[0]].shape[1]
    parts = {
        z: jnp.concatenate([ref[natom + 16 * j : natom + 16 * (j + 1), :] for j in range(natom // width)], 1)
        for z, ref in zb.items()
    }
    phases = {}
    for z, t in pairs:
        table = tables[t][(t % 2) * nk : (t % 2 + 1) * nk, :]
        phases[z, t] = jnp.dot(table, parts[z], preferred_element_type=f32)
    cot = {z: ref[0:natom, :] for z, ref in zb.items()}
    step = 32
    for b, t in enumerate(blocks):
        for i in range(0, nk, step):
            sums = [None, None]
            for z in atoms:
                for k, value in enumerate(cos_sin(phases[z, t][i : i + step])):
                    value = value.astype(bf16)
                    tiles[z, t][k * nk + i : k * nk + i + step, :] = value
                    part = jnp.dot(value, cot[z], preferred_element_type=f32)
                    sums[k] = part if sums[k] is None else sums[k] + part
            for k, total in enumerate(sums):
                row = k * nk + i
                if started:
                    total = total + before[t][row : row + step, :]
                if last:
                    outs[0][2 * nk * b + row : 2 * nk * b + row + step, :] = total.astype(outs[0].dtype)
                else:
                    outs[b][row : row + step, :] = total


def shuffled(ref, flip, half, nk):
    rows = [ref[2 * nk * (t ^ flip) : 2 * nk * ((t ^ flip) + 1), :] for t in range(half)]
    return jnp.concatenate(rows, 0).astype(f32)


def pair_body(own_ref, got_ref, f_ref, fb_ref):
    total = own_ref[...] + got_ref[...].astype(f32)
    f_ref[...] = total
    fb_ref[...] = total.astype(bf16)


def weight_body(half, nk, flips, scale, *refs):
    total = refs[0][...]
    for ref, flip in zip(refs[1:], flips):
        total = total + shuffled(ref, flip // 2, half, nk)
    total = total * scale
    fb = refs[1 + len(flips) : 1 + len(flips) + half]
    weight_ref, head_ref = refs[1 + len(flips) + half :]
    for t in range(half):
        fil = fb[t][...]
        rows = total[2 * nk * t : 2 * nk * (t + 1)] * jnp.concatenate([fil, fil], 0)
        weight_ref[:, 2 * nk * t : 2 * nk * (t + 1)] = rows.T.astype(bf16)
    head_ref[...] = total[0 : 2 * nk]


def part_of(weight_ref, tiles):
    tile = jnp.concatenate([ref[...] for ref in tiles], 0)
    return jnp.dot(weight_ref[...], tile, preferred_element_type=f32)


def mine_body(nz, half, weight_ref, *refs):
    for z in range(nz):
        refs[nz * half + z][...] = part_of(weight_ref, refs[z * half : (z + 1) * half])


def node_body(half, part_ref, weight_ref, *refs):
    total = part_ref[...] + part_of(weight_ref, refs[:half])
    refs[half][...] = total.T.astype(refs[half].dtype)


def own_body(half, head_ref, saved_ref, part_ref, weight_ref, *refs):
    node_body(half, part_ref, weight_ref, *refs)
    grad_ref = refs[half + 1]
    nk = grad_ref.shape[0]
    grad_ref[...] = head_ref[0:nk] * saved_ref[0] + head_ref[nk : 2 * nk] * saved_ref[1]


def final_body(scale, *refs):
    total = refs[0][...]
    for ref in refs[1:-1]:
        total = total + ref[...].astype(f32)
    refs[-1][...] = (total * scale).astype(bf16)


def shape(dims, kind):
    return jax.ShapeDtypeStruct(dims, kind)


def local(lattice, positions, cotangent, filters, saved_factor):
    nz = lax.axis_size("atoms")
    nq = lax.axis_size("kvec")
    natom, width = cotangent.shape
    nk = lattice.shape[1]
    half = nq // 2
    count = half * nk
    scale_n = 1.0 / math.sqrt(natom * nz * nq)
    scale_k = 1.0 / math.sqrt(nk * nz * nq)
    keep = nz * natom * 4 * count * 2 <= VMEM_BUDGET

    def swap(value, flip):
        return lax.ppermute(value, "kvec", [(i, i ^ flip) for i in range(nq)])

    def shift(value, by):
        return lax.ppermute(value, "atoms", [(i, (i + by) % nz) for i in range(nz)])

    def run(body, outs, *args, keep_args=keep, keep_outs=keep):
        return call(body, outs, *args, keep_args=keep_args, keep_outs=keep_outs)

    zbuf, wide = run(
        pack_body,
        [shape((natom + 16 * (natom // width), width), bf16), shape((8, width), f32)],
        lattice,
        positions,
        cotangent,
        keep_args=False,
    )
    ring = gather_order(nz)
    flips = list(range(2, nq, 2))
    zb = {0: zbuf}
    for d in ring:
        zb[d] = shift(zbuf, -d)
    (cores,) = run(join_body, [shape((16, width), f32)], wide, swap(wide, 1))
    lats = [cores] + [swap(cores, s) for s in flips]
    fils = [filters] + [swap(filters, s) for s in flips]
    table = {}
    for s, lat in zip([0] + flips, lats):
        (both,) = run(lambda *refs: table_body(nk, *refs), [shape((2 * nk, 16), bf16)], lat)
        table[s] = table[s + 1] = both
    mine = list(range(0, nq, 2))
    theirs = list(range(1, nq, 2))
    tiles = {}
    total = {}

    def factor(atoms, blocks, last=None):
        pairs = [(z, t) for z in sorted(atoms) for t in blocks]
        outs = [shape((2 * nk, natom), bf16)] * len(pairs)
        if last is None:
            outs += [shape((2 * nk, width), f32)] * len(blocks)
        else:
            outs.append(shape((2 * nk * len(blocks), width), last))
        started = blocks[0] in total
        args = [zb[z] for z in sorted(atoms)] + [table[t] for t in blocks] + [total[t] for t in blocks if started]
        body = lambda *refs: factor_body(natom, nk, pairs, blocks, started, last is not None, *refs)
        got = run(body, outs, *args)
        tiles.update(zip(pairs, got))
        if last is None:
            total.update(zip(blocks, got[len(pairs) :]))
        return got[-1]

    order = [0] + ring
    early = order[: min(2, len(order) - 1)]
    for z in early:
        factor([z], [0, 1])
    for t in flips:
        factor(early, [t, t + 1])
    for z in order[len(early) : -1]:
        factor([z], list(range(nq)))
    sent = factor(order[-1:], theirs, bf16)
    kept = factor(order[-1:], mine, f32)
    pair, pair16 = run(
        pair_body,
        [shape((2 * count, width), f32), shape((2 * count, width), bf16)],
        kept,
        swap(sent, 1),
    )
    got = [swap(pair16, s) for s in flips]
    weight, head = run(
        lambda *refs: weight_body(half, nk, flips, scale_n, *refs),
        [shape((width, 2 * count), bf16), shape((2 * nk, width), f32)],
        pair,
        *got,
        *fils,
    )
    other = swap(weight, 1)
    parts = run(
        lambda *refs: mine_body(nz, half, *refs),
        [shape((width, natom), f32)] * nz,
        weight,
        *[tiles[s, t] for s in order for t in mine],
    )
    parts = dict(zip(order, parts))
    landed = []
    for d in range(1, nz):
        (node,) = run(
            lambda *refs: node_body(half, *refs),
            [shape((natom, width), bf16)],
            parts[d],
            other,
            *[tiles[d, t] for t in theirs],
        )
        landed.append(shift(node, d))
    own, filter_grad = run(
        lambda *refs: own_body(half, *refs),
        [shape((natom, width), f32), shape((nk, width), f32)],
        head,
        saved_factor,
        parts[0],
        other,
        *[tiles[0, t] for t in theirs],
    )
    (node_grad,) = run(
        lambda *refs: final_body(scale_k, *refs),
        [shape((natom, width), bf16)],
        own,
        *landed,
        keep_outs=False,
    )
    return (node_grad, filter_grad)


def gather_order(nz):
    order = []
    for d in range(1, nz // 2 + 1):
        order += [nz - d, d] if nz - d != d else [d]
    return [d for d in order if d]


def solution(mesh):
    in_specs = (
        P(None, ("atoms", "kvec")),
        P(None, ("beads", "atoms", "kvec")),
        P(("beads", "atoms", "kvec"), None),
        P(("atoms", "kvec"), None),
        P(None, ("beads", "atoms", "kvec"), None),
    )
    out_specs = (P(("beads", "atoms", "kvec"), None), P(("beads", "atoms", "kvec"), None))
    return jax.shard_map(local, mesh=mesh, in_specs=in_specs, out_specs=out_specs, check_vma=False)
```

```python
import math

import jax
import jax.numpy as jnp
from jax import lax
from jax.experimental import pallas as pl
from jax.experimental.pallas import tpu as pltpu
from jax.sharding import PartitionSpec as P


f32 = jnp.float32
bf16 = jnp.bfloat16


SIN_COEF = None
COS_COEF = None


def _fit():
    import numpy as np

    n = 4001
    t = np.cos(np.pi * (np.arange(n) + 0.5) / n)
    u = (t + 1.0) * 0.125
    r = np.sqrt(u)
    root = math.sqrt(2.0)
    sin_ratio = np.where(r > 1e-9, root * np.sin(np.pi * r) / np.maximum(r, 1e-9), root * np.pi)
    cheb = np.polynomial.chebyshev.Chebyshev
    s = cheb.fit(u, sin_ratio, 4, domain=[0.0, 0.25]).convert(kind=np.polynomial.Polynomial)
    c = cheb.fit(u, root * np.cos(np.pi * r), 4, domain=[0.0, 0.25]).convert(kind=np.polynomial.Polynomial)
    return tuple(float(v) for v in s.coef), tuple(float(v) for v in c.coef)


SIN_COEF, COS_COEF = _fit()


def _horner(coef, u):
    acc = jnp.full_like(u, coef[-1])
    for value in coef[-2::-1]:
        acc = acc * u + value
    return acc


def cos_sin(phase):
    r = phase - jnp.round(phase)
    u = r * r
    s = r * _horner(SIN_COEF, u)
    c = _horner(COS_COEF, u)
    return 1.0 - s * s, s * c


def full_spec(count):
    return [pl.BlockSpec(memory_space=pltpu.VMEM)] * count


VMEM_BUDGET = 4 * 1024 * 1024


def call(body, outs, *args, keep_args=True, keep_outs=True):
    if keep_args:
        args = [pltpu.with_memory_space_constraint(arg, pltpu.VMEM) for arg in args]
    if keep_outs:
        outs = [pltpu.VMEM(v.shape, v.dtype) for v in outs]
    return pl.pallas_call(
        body,
        out_shape=outs,
        in_specs=full_spec(len(args)),
        out_specs=full_spec(len(outs)),
    )(*args)


def pack_body(lat_hbm, pos_hbm, cot_hbm, fil_hbm, out_ref, wide_ref, fil_ref, lat_ref, pos_ref, sem):
    natom, width = cot_hbm.shape
    nk = lat_ref.shape[1]
    copies = [
        pltpu.make_async_copy(pos_hbm, pos_ref, sem.at[0]),
        pltpu.make_async_copy(lat_hbm, lat_ref, sem.at[1]),
        pltpu.make_async_copy(cot_hbm, out_ref.at[pl.ds(0, natom)], sem.at[2]),
        pltpu.make_async_copy(fil_hbm, fil_ref, sem.at[3]),
    ]
    for copy in copies:
        copy.start()
    copies[0].wait()
    x = pos_ref[...]
    hi = x.astype(bf16).astype(f32)
    rest = x - hi
    mid = rest.astype(bf16).astype(f32)
    low = rest - mid
    zero = jnp.zeros_like(x)
    parts = jnp.concatenate([hi, mid, low, zero, zero, zero[:1]], 0).astype(bf16)
    for j in range(natom // width):
        out_ref[natom + 16 * j : natom + 16 * (j + 1), :] = parts[:, j * width : (j + 1) * width]
    copies[1].wait()
    row = lax.broadcasted_iota(jnp.int32, (nk, width), 0)
    col = lax.broadcasted_iota(jnp.int32, (nk, width), 1)
    spread = (row == col % nk).astype(bf16)
    lat = lat_ref[...].astype(f32).astype(bf16)
    wide = jnp.dot(lat, spread, preferred_element_type=f32)
    wide_ref[...] = jnp.concatenate([wide, wide, wide[:2]], 0)
    copies[2].wait()
    copies[3].wait()


def pack(keep, lattice, positions, cotangent, filters):
    natom, width = cotangent.shape
    outs = [shape((natom + 16 * (natom // width), width), bf16), shape((8, width), f32), shape(filters.shape, f32)]
    if keep:
        outs = [pltpu.VMEM(v.shape, v.dtype) for v in outs]
    return pl.pallas_call(
        pack_body,
        out_shape=outs,
        in_specs=[pl.BlockSpec(memory_space=pl.ANY)] * 4,
        out_specs=full_spec(3),
        scratch_shapes=[
            pltpu.VMEM(lattice.shape, lattice.dtype),
            pltpu.VMEM(positions.shape, positions.dtype),
            pltpu.SemaphoreType.DMA((4,)),
        ],
    )(lattice, positions, cotangent, filters)


def join_body(own_ref, got_ref, out_ref):
    out_ref[0:8, :] = own_ref[...]
    out_ref[8:16, :] = got_ref[...]


def table_body(nk, lat_ref, out_ref):
    width = lat_ref.shape[1]
    zero = jnp.zeros((3, width), f32)
    for h in range(2):
        lat = lat_ref[8 * h : 8 * h + 3, :]
        cols = jnp.concatenate([lat, lat, lat, zero, zero, zero[:1]], 0).T
        out_ref[h * nk : (h + 1) * nk, :] = cols[0:nk].astype(bf16)


def factor_body(natom, nk, pairs, blocks, started, last, *refs):
    atoms = sorted({z for z, t in pairs})
    zb, refs = dict(zip(atoms, refs)), refs[len(atoms) :]
    tables, refs = dict(zip(blocks, refs)), refs[len(blocks) :]
    before, refs = (dict(zip(blocks, refs)), refs[len(blocks) :]) if started else ({}, refs)
    tiles, outs = dict(zip(pairs, refs)), refs[len(pairs) :]
    width = zb[atoms[0]].shape[1]
    parts = {
        z: jnp.concatenate([ref[natom + 16 * j : natom + 16 * (j + 1), :] for j in range(natom // width)], 1)
        for z, ref in zb.items()
    }
    phases = {}
    for z, t in pairs:
        table = tables[t][(t % 2) * nk : (t % 2 + 1) * nk, :]
        phases[z, t] = jnp.dot(table, parts[z], preferred_element_type=f32)
    cot = {z: ref[0:natom, :] for z, ref in zb.items()}
    step = 32
    for b, t in enumerate(blocks):
        for i in range(0, nk, step):
            sums = [None, None]
            for z in atoms:
                for k, value in enumerate(cos_sin(phases[z, t][i : i + step])):
                    value = value.astype(bf16)
                    tiles[z, t][k * nk + i : k * nk + i + step, :] = value
                    part = jnp.dot(value, cot[z], preferred_element_type=f32)
                    sums[k] = part if sums[k] is None else sums[k] + part
            for k, total in enumerate(sums):
                row = k * nk + i
                if started:
                    total = total + before[t][row : row + step, :]
                if last:
                    outs[0][2 * nk * b + row : 2 * nk * b + row + step, :] = total.astype(outs[0].dtype)
                else:
                    outs[b][row : row + step, :] = total


def shuffled(ref, flip, half, nk):
    rows = [ref[2 * nk * (t ^ flip) : 2 * nk * ((t ^ flip) + 1), :] for t in range(half)]
    return jnp.concatenate(rows, 0).astype(f32)


def pair_body(own_ref, got_ref, f_ref, fb_ref):
    total = own_ref[...] + got_ref[...].astype(f32)
    f_ref[...] = total
    fb_ref[...] = total.astype(bf16)


def weight_body(half, nk, flips, scale, *refs):
    total = refs[0][...]
    for ref, flip in zip(refs[1:], flips):
        total = total + shuffled(ref, flip // 2, half, nk)
    total = total * scale
    fb = refs[1 + len(flips) : 1 + len(flips) + half]
    weight_ref, head_ref = refs[1 + len(flips) + half :]
    for t in range(half):
        fil = fb[t][...]
        rows = total[2 * nk * t : 2 * nk * (t + 1)] * jnp.concatenate([fil, fil], 0)
        weight_ref[:, 2 * nk * t : 2 * nk * (t + 1)] = rows.T.astype(bf16)
    head_ref[...] = total[0 : 2 * nk]


def part_of(weight_ref, tiles):
    tile = jnp.concatenate([ref[...] for ref in tiles], 0)
    return jnp.dot(weight_ref[...], tile, preferred_element_type=f32)


def mine_body(nz, half, weight_ref, *refs):
    for z in range(nz):
        refs[nz * half + z][...] = part_of(weight_ref, refs[z * half : (z + 1) * half])


def node_body(half, part_ref, weight_ref, *refs):
    total = part_ref[...] + part_of(weight_ref, refs[:half])
    refs[half][...] = total.T.astype(refs[half].dtype)


def own_body(half, head_ref, saved_ref, part_ref, weight_ref, *refs):
    node_body(half, part_ref, weight_ref, *refs)
    grad_ref = refs[half + 1]
    nk = grad_ref.shape[0]
    grad_ref[...] = head_ref[0:nk] * saved_ref[0] + head_ref[nk : 2 * nk] * saved_ref[1]


def final_body(scale, *refs):
    total = refs[0][...]
    for ref in refs[1:-1]:
        total = total + ref[...].astype(f32)
    refs[-1][...] = (total * scale).astype(bf16)


def shape(dims, kind):
    return jax.ShapeDtypeStruct(dims, kind)


def local(lattice, positions, cotangent, filters, saved_factor):
    nz = lax.axis_size("atoms")
    nq = lax.axis_size("kvec")
    natom, width = cotangent.shape
    nk = lattice.shape[1]
    half = nq // 2
    count = half * nk
    scale_n = 1.0 / math.sqrt(natom * nz * nq)
    scale_k = 1.0 / math.sqrt(nk * nz * nq)
    keep = nz * natom * 4 * count * 2 <= VMEM_BUDGET

    def swap(value, flip):
        return lax.ppermute(value, "kvec", [(i, i ^ flip) for i in range(nq)])

    def shift(value, by):
        return lax.ppermute(value, "atoms", [(i, (i + by) % nz) for i in range(nz)])

    def run(body, outs, *args, keep_args=keep, keep_outs=keep):
        return call(body, outs, *args, keep_args=keep_args, keep_outs=keep_outs)

    zbuf, wide, filters = pack(keep, lattice, positions, cotangent, filters)
    ring = gather_order(nz)
    flips = list(range(2, nq, 2))
    zb = {0: zbuf}
    for d in ring:
        zb[d] = shift(zbuf, -d)
    (cores,) = run(join_body, [shape((16, width), f32)], wide, swap(wide, 1))
    lats = [cores] + [swap(cores, s) for s in flips]
    fils = [filters] + [swap(filters, s) for s in flips]
    table = {}
    for s, lat in zip([0] + flips, lats):
        (both,) = run(lambda *refs: table_body(nk, *refs), [shape((2 * nk, 16), bf16)], lat)
        table[s] = table[s + 1] = both
    mine = list(range(0, nq, 2))
    theirs = list(range(1, nq, 2))
    tiles = {}
    total = {}

    def factor(atoms, blocks, last=None):
        pairs = [(z, t) for z in sorted(atoms) for t in blocks]
        outs = [shape((2 * nk, natom), bf16)] * len(pairs)
        if last is None:
            outs += [shape((2 * nk, width), f32)] * len(blocks)
        else:
            outs.append(shape((2 * nk * len(blocks), width), last))
        started = blocks[0] in total
        args = [zb[z] for z in sorted(atoms)] + [table[t] for t in blocks] + [total[t] for t in blocks if started]
        body = lambda *refs: factor_body(natom, nk, pairs, blocks, started, last is not None, *refs)
        got = run(body, outs, *args)
        tiles.update(zip(pairs, got))
        if last is None:
            total.update(zip(blocks, got[len(pairs) :]))
        return got[-1]

    order = [0] + ring
    early = order[: min(3, len(order) - 1)]
    for z in early:
        factor([z], [0, 1])
    for t in flips:
        factor(early, [t, t + 1])
    for z in order[len(early) : -1]:
        factor([z], list(range(nq)))
    sent = factor(order[-1:], theirs, bf16)
    kept = factor(order[-1:], mine, f32)
    pair, pair16 = run(
        pair_body, [shape((2 * count, width), f32), shape((2 * count, width), bf16)], kept, swap(sent, 1)
    )
    got = [swap(pair16, s) for s in flips]
    weight, head = run(
        lambda *refs: weight_body(half, nk, flips, scale_n, *refs),
        [shape((width, 2 * count), bf16), shape((2 * nk, width), f32)],
        pair,
        *got,
        *fils,
    )
    other = swap(weight, 1)
    parts = run(
        lambda *refs: mine_body(nz, half, *refs),
        [shape((width, natom), f32)] * nz,
        weight,
        *[tiles[s, t] for s in order for t in mine],
    )
    parts = dict(zip(order, parts))
    landed = []
    for d in range(1, nz):
        (node,) = run(
            lambda *refs: node_body(half, *refs),
            [shape((natom, width), bf16)],
            parts[d],
            other,
            *[tiles[d, t] for t in theirs],
        )
        landed.append(shift(node, d))
    own, filter_grad = run(
        lambda *refs: own_body(half, *refs),
        [shape((natom, width), f32), shape((nk, width), f32)],
        head,
        saved_factor,
        parts[0],
        other,
        *[tiles[0, t] for t in theirs],
    )
    (node_grad,) = run(
        lambda *refs: final_body(scale_k, *refs), [shape((natom, width), bf16)], own, *landed, keep_outs=False
    )
    return (node_grad, filter_grad)


def gather_order(nz):
    order = []
    for d in range(1, nz // 2 + 1):
        order += [nz - d, d] if nz - d != d else [d]
    return [d for d in order if d]


def solution(mesh):
    in_specs = (
        P(None, ("atoms", "kvec")),
        P(None, ("beads", "atoms", "kvec")),
        P(("beads", "atoms", "kvec"), None),
        P(("atoms", "kvec"), None),
        P(None, ("beads", "atoms", "kvec"), None),
    )
    out_specs = (P(("beads", "atoms", "kvec"), None), P(("beads", "atoms", "kvec"), None))
    return jax.shard_map(local, mesh=mesh, in_specs=in_specs, out_specs=out_specs, check_vma=False)
```

```python
import math

import jax
import jax.numpy as jnp
from jax import lax
from jax.experimental import pallas as pl
from jax.experimental.pallas import tpu as pltpu
from jax.sharding import PartitionSpec as P


f32 = jnp.float32
bf16 = jnp.bfloat16


SIN_COEF = None
COS_COEF = None


def _fit():
    import numpy as np

    n = 4001
    t = np.cos(np.pi * (np.arange(n) + 0.5) / n)
    u = (t + 1.0) * 0.125
    r = np.sqrt(u)
    root = math.sqrt(2.0)
    sin_ratio = np.where(r > 1e-9, root * np.sin(np.pi * r) / np.maximum(r, 1e-9), root * np.pi)
    cheb = np.polynomial.chebyshev.Chebyshev
    s = cheb.fit(u, sin_ratio, 4, domain=[0.0, 0.25]).convert(kind=np.polynomial.Polynomial)
    c = cheb.fit(u, root * np.cos(np.pi * r), 4, domain=[0.0, 0.25]).convert(kind=np.polynomial.Polynomial)
    return tuple(float(v) for v in s.coef), tuple(float(v) for v in c.coef)


SIN_COEF, COS_COEF = _fit()


def _horner(coef, u):
    acc = jnp.full_like(u, coef[-1])
    for value in coef[-2::-1]:
        acc = acc * u + value
    return acc


def cos_sin(phase):
    r = phase - jnp.round(phase)
    u = r * r
    s = r * _horner(SIN_COEF, u)
    c = _horner(COS_COEF, u)
    return 1.0 - s * s, s * c


def full_spec(count):
    return [pl.BlockSpec(memory_space=pltpu.VMEM)] * count


VMEM_BUDGET = 4 * 1024 * 1024


def call(body, outs, *args, keep_args=True, keep_outs=True):
    if keep_args:
        args = [pltpu.with_memory_space_constraint(arg, pltpu.VMEM) for arg in args]
    if keep_outs:
        outs = [pltpu.VMEM(v.shape, v.dtype) for v in outs]
    return pl.pallas_call(
        body,
        out_shape=outs,
        in_specs=full_spec(len(args)),
        out_specs=full_spec(len(outs)),
    )(*args)


def pack_body(lat_hbm, pos_hbm, cot_hbm, fil_hbm, out_ref, wide_ref, fil_ref, lat_ref, pos_ref, sem):
    natom, width = cot_hbm.shape
    nk = lat_ref.shape[1]
    copies = [
        pltpu.make_async_copy(pos_hbm, pos_ref, sem.at[0]),
        pltpu.make_async_copy(lat_hbm, lat_ref, sem.at[1]),
        pltpu.make_async_copy(cot_hbm, out_ref.at[pl.ds(0, natom)], sem.at[2]),
        pltpu.make_async_copy(fil_hbm, fil_ref, sem.at[3]),
    ]
    for copy in copies:
        copy.start()
    copies[0].wait()
    x = pos_ref[...]
    hi = x.astype(bf16).astype(f32)
    rest = x - hi
    mid = rest.astype(bf16).astype(f32)
    low = rest - mid
    zero = jnp.zeros_like(x)
    parts = jnp.concatenate([hi, mid, low, zero, zero, zero[:1]], 0).astype(bf16)
    for j in range(natom // width):
        out_ref[natom + 16 * j : natom + 16 * (j + 1), :] = parts[:, j * width : (j + 1) * width]
    copies[1].wait()
    row = lax.broadcasted_iota(jnp.int32, (nk, width), 0)
    col = lax.broadcasted_iota(jnp.int32, (nk, width), 1)
    spread = (row == col % nk).astype(bf16)
    lat = lat_ref[...].astype(f32).astype(bf16)
    wide = jnp.dot(lat, spread, preferred_element_type=f32)
    wide_ref[...] = jnp.concatenate([wide, wide, wide[:2]], 0)
    copies[2].wait()
    copies[3].wait()


def pack(keep, lattice, positions, cotangent, filters):
    natom, width = cotangent.shape
    outs = [shape((natom + 16 * (natom // width), width), bf16), shape((8, width), f32), shape(filters.shape, f32)]
    if keep:
        outs = [pltpu.VMEM(v.shape, v.dtype) for v in outs]
    return pl.pallas_call(
        pack_body,
        out_shape=outs,
        in_specs=[pl.BlockSpec(memory_space=pl.ANY)] * 4,
        out_specs=full_spec(3),
        scratch_shapes=[
            pltpu.VMEM(lattice.shape, lattice.dtype),
            pltpu.VMEM(positions.shape, positions.dtype),
            pltpu.SemaphoreType.DMA((4,)),
        ],
    )(lattice, positions, cotangent, filters)


def join_body(own_ref, got_ref, out_ref):
    out_ref[0:8, :] = own_ref[...]
    out_ref[8:16, :] = got_ref[...]


def table_body(nk, lat_ref, out_ref):
    width = lat_ref.shape[1]
    zero = jnp.zeros((3, width), f32)
    for h in range(2):
        lat = lat_ref[8 * h : 8 * h + 3, :]
        cols = jnp.concatenate([lat, lat, lat, zero, zero, zero[:1]], 0).T
        out_ref[h * nk : (h + 1) * nk, :] = cols[0:nk].astype(bf16)


def factor_body(natom, nk, pairs, blocks, started, last, *refs):
    atoms = sorted({z for z, t in pairs})
    zb, refs = dict(zip(atoms, refs)), refs[len(atoms) :]
    tables, refs = dict(zip(blocks, refs)), refs[len(blocks) :]
    before, refs = (dict(zip(blocks, refs)), refs[len(blocks) :]) if started else ({}, refs)
    tiles, outs = dict(zip(pairs, refs)), refs[len(pairs) :]
    width = zb[atoms[0]].shape[1]
    parts = {
        z: jnp.concatenate([ref[natom + 16 * j : natom + 16 * (j + 1), :] for j in range(natom // width)], 1)
        for z, ref in zb.items()
    }
    phases = {}
    for z, t in pairs:
        table = tables[t][(t % 2) * nk : (t % 2 + 1) * nk, :]
        phases[z, t] = jnp.dot(table, parts[z], preferred_element_type=f32)
    cot = {z: ref[0:natom, :] for z, ref in zb.items()}
    step = 32
    for b, t in enumerate(blocks):
        for i in range(0, nk, step):
            sums = [None, None]
            for z in atoms:
                for k, value in enumerate(cos_sin(phases[z, t][i : i + step])):
                    value = value.astype(bf16)
                    tiles[z, t][k * nk + i : k * nk + i + step, :] = value
                    part = jnp.dot(value, cot[z], preferred_element_type=f32)
                    sums[k] = part if sums[k] is None else sums[k] + part
            for k, total in enumerate(sums):
                row = k * nk + i
                if started:
                    total = total + before[t][row : row + step, :]
                if last:
                    outs[0][2 * nk * b + row : 2 * nk * b + row + step, :] = total.astype(outs[0].dtype)
                else:
                    outs[b][row : row + step, :] = total


def shuffled(ref, flip, half, nk):
    rows = [ref[2 * nk * (t ^ flip) : 2 * nk * ((t ^ flip) + 1), :] for t in range(half)]
    return jnp.concatenate(rows, 0).astype(f32)


def pair_body(own_ref, got_ref, f_ref, fb_ref):
    total = own_ref[...] + got_ref[...].astype(f32)
    f_ref[...] = total
    fb_ref[...] = total.astype(bf16)


def weight_body(half, nk, flips, scale, *refs):
    total = refs[0][...]
    for ref, flip in zip(refs[1:], flips):
        total = total + shuffled(ref, flip // 2, half, nk)
    total = total * scale
    fb = refs[1 + len(flips) : 1 + len(flips) + half]
    weight_ref, head_ref = refs[1 + len(flips) + half :]
    for t in range(half):
        fil = fb[t][...]
        rows = total[2 * nk * t : 2 * nk * (t + 1)] * jnp.concatenate([fil, fil], 0)
        weight_ref[:, 2 * nk * t : 2 * nk * (t + 1)] = rows.T.astype(bf16)
    head_ref[...] = total[0 : 2 * nk]


def part_of(weight_ref, tiles):
    tile = jnp.concatenate([ref[...] for ref in tiles], 0)
    return jnp.dot(weight_ref[...], tile, preferred_element_type=f32)


def mine_body(nz, half, weight_ref, *refs):
    for z in range(nz):
        refs[nz * half + z][...] = part_of(weight_ref, refs[z * half : (z + 1) * half])


def node_body(half, choices, *refs):
    weight_ref, refs = refs[0], refs[1:]
    out_ref = refs[-1]

    def one(part_ref, *tiles):
        total = part_ref[...] + part_of(weight_ref, tiles)
        out_ref[...] = total.T.astype(out_ref.dtype)

    groups = [refs[i * (half + 1) : (i + 1) * (half + 1)] for i in range(len(choices))]
    if len(choices) == 1:
        one(*groups[0])
        return
    plane = lax.axis_index("atoms")
    for planes, group in zip(choices, groups):
        taken = plane == planes[0]
        for other in planes[1:]:
            taken = taken | (plane == other)
        pl.when(taken)(lambda group=group: one(*group))


def own_body(half, head_ref, saved_ref, weight_ref, *refs):
    node_body(half, [None], weight_ref, *refs[:-1])
    grad_ref = refs[-1]
    nk = grad_ref.shape[0]
    grad_ref[...] = head_ref[0:nk] * saved_ref[0] + head_ref[nk : 2 * nk] * saved_ref[1]


def final_body(scale, *refs):
    total = refs[0][...]
    for ref in refs[1:-1]:
        total = total + ref[...].astype(f32)
    refs[-1][...] = (total * scale).astype(bf16)


def shape(dims, kind):
    return jax.ShapeDtypeStruct(dims, kind)


def local(lattice, positions, cotangent, filters, saved_factor):
    nz = lax.axis_size("atoms")
    nq = lax.axis_size("kvec")
    natom, width = cotangent.shape
    nk = lattice.shape[1]
    half = nq // 2
    count = half * nk
    scale_n = 1.0 / math.sqrt(natom * nz * nq)
    scale_k = 1.0 / math.sqrt(nk * nz * nq)
    keep = nz * natom * 4 * count * 2 <= VMEM_BUDGET

    def swap(value, flip):
        return lax.ppermute(value, "kvec", [(i, i ^ flip) for i in range(nq)])

    def send(value, targets):
        return lax.ppermute(value, "atoms", list(enumerate(targets)))

    def run(body, outs, *args, keep_args=keep, keep_outs=keep):
        return call(body, outs, *args, keep_args=keep_args, keep_outs=keep_outs)

    zbuf, wide, filters = pack(keep, lattice, positions, cotangent, filters)
    ring = gather_order(nz)
    flips = list(range(2, nq, 2))
    zb = {0: zbuf}
    for d in ring:
        zb[d] = send(zbuf, [(i - d) % nz for i in range(nz)])
    (cores,) = run(join_body, [shape((16, width), f32)], wide, swap(wide, 1))
    lats = [cores] + [swap(cores, s) for s in flips]
    fils = [filters] + [swap(filters, s) for s in flips]
    table = {}
    for s, lat in zip([0] + flips, lats):
        (both,) = run(lambda *refs: table_body(nk, *refs), [shape((2 * nk, 16), bf16)], lat)
        table[s] = table[s + 1] = both
    mine = list(range(0, nq, 2))
    theirs = list(range(1, nq, 2))
    tiles = {}
    total = {}

    def factor(atoms, blocks, last=None):
        pairs = [(z, t) for z in sorted(atoms) for t in blocks]
        outs = [shape((2 * nk, natom), bf16)] * len(pairs)
        if last is None:
            outs += [shape((2 * nk, width), f32)] * len(blocks)
        else:
            outs.append(shape((2 * nk * len(blocks), width), last))
        started = blocks[0] in total
        args = [zb[z] for z in sorted(atoms)] + [table[t] for t in blocks] + [total[t] for t in blocks if started]
        body = lambda *refs: factor_body(natom, nk, pairs, blocks, started, last is not None, *refs)
        got = run(body, outs, *args)
        tiles.update(zip(pairs, got))
        if last is None:
            total.update(zip(blocks, got[len(pairs) :]))
        return got[-1]

    order = [0] + ring
    early = order[: min(3, len(order) - 1)]
    for z in early:
        factor([z], [0, 1])
    for t in flips:
        factor(early, [t, t + 1])
    for z in order[len(early) : -1]:
        factor([z], list(range(nq)))
    sent = factor(order[-1:], theirs, bf16)
    kept = factor(order[-1:], mine, f32)
    pair, pair16 = run(
        pair_body, [shape((2 * count, width), f32), shape((2 * count, width), bf16)], kept, swap(sent, 1)
    )
    got = [swap(pair16, s) for s in flips]
    weight, head = run(
        lambda *refs: weight_body(half, nk, flips, scale_n, *refs),
        [shape((width, 2 * count), bf16), shape((2 * nk, width), f32)],
        pair,
        *got,
        *fils,
    )
    other = swap(weight, 1)
    parts = run(
        lambda *refs: mine_body(nz, half, *refs),
        [shape((width, natom), f32)] * nz,
        weight,
        *[tiles[s, t] for s in order for t in mine],
    )
    parts = dict(zip(order, parts))
    landed = []
    for targets in reduce_rounds(nz):
        planes = {}
        for i, target in enumerate(targets):
            planes.setdefault((target - i) % nz, []).append(i)
        (node,) = run(
            lambda *refs: node_body(half, list(planes.values()), *refs),
            [shape((natom, width), bf16)],
            other,
            *[v for d in planes for v in [parts[d], *[tiles[d, t] for t in theirs]]],
        )
        landed.append(send(node, targets))
    own, filter_grad = run(
        lambda *refs: own_body(half, *refs),
        [shape((natom, width), f32), shape((nk, width), f32)],
        head,
        saved_factor,
        other,
        parts[0],
        *[tiles[0, t] for t in theirs],
    )
    (node_grad,) = run(
        lambda *refs: final_body(scale_k, *refs), [shape((natom, width), bf16)], own, *landed, keep_outs=False
    )
    return (node_grad, filter_grad)


def gather_order(nz):
    return list(range(nz - 1, 0, -1))


def reduce_rounds(nz):
    ring = list(range(nz))
    if nz <= 4:
        ring = ring[:1] + ring[1::2] + ring[2::2][::-1]
    place = {z: i for i, z in enumerate(ring)}
    return [[ring[(place[z] + by) % nz] for z in range(nz)] for by in range(1, nz)]


def solution(mesh):
    in_specs = (
        P(None, ("atoms", "kvec")),
        P(None, ("beads", "atoms", "kvec")),
        P(("beads", "atoms", "kvec"), None),
        P(("atoms", "kvec"), None),
        P(None, ("beads", "atoms", "kvec"), None),
    )
    out_specs = (P(("beads", "atoms", "kvec"), None), P(("beads", "atoms", "kvec"), None))
    return jax.shard_map(local, mesh=mesh, in_specs=in_specs, out_specs=out_specs, check_vma=False)
```

```python
import math

import jax
import jax.numpy as jnp
from jax import lax
from jax.experimental import pallas as pl
from jax.experimental.pallas import tpu as pltpu
from jax.sharding import PartitionSpec as P


f32 = jnp.float32
bf16 = jnp.bfloat16


SIN_COEF = None
COS_COEF = None


def _fit():
    import numpy as np

    n = 4001
    t = np.cos(np.pi * (np.arange(n) + 0.5) / n)
    u = (t + 1.0) * 0.125
    r = np.sqrt(u)
    root = math.sqrt(2.0)
    sin_ratio = np.where(r > 1e-9, root * np.sin(np.pi * r) / np.maximum(r, 1e-9), root * np.pi)
    cheb = np.polynomial.chebyshev.Chebyshev
    s = cheb.fit(u, sin_ratio, 4, domain=[0.0, 0.25]).convert(kind=np.polynomial.Polynomial)
    c = cheb.fit(u, root * np.cos(np.pi * r), 4, domain=[0.0, 0.25]).convert(kind=np.polynomial.Polynomial)
    return tuple(float(v) for v in s.coef), tuple(float(v) for v in c.coef)


SIN_COEF, COS_COEF = _fit()


def _horner(coef, u):
    acc = jnp.full_like(u, coef[-1])
    for value in coef[-2::-1]:
        acc = acc * u + value
    return acc


def cos_sin(phase):
    r = phase - jnp.round(phase)
    u = r * r
    s = r * _horner(SIN_COEF, u)
    c = _horner(COS_COEF, u)
    return 1.0 - s * s, s * c


def full_spec(count):
    return [pl.BlockSpec(memory_space=pltpu.VMEM)] * count


VMEM_BUDGET = 4 * 1024 * 1024


def call(body, outs, *args, keep_args=True, keep_outs=True):
    if keep_args:
        args = [pltpu.with_memory_space_constraint(arg, pltpu.VMEM) for arg in args]
    if keep_outs:
        outs = [pltpu.VMEM(v.shape, v.dtype) for v in outs]
    return pl.pallas_call(
        body,
        out_shape=outs,
        in_specs=full_spec(len(args)),
        out_specs=full_spec(len(outs)),
    )(*args)


def pack_body(lat_hbm, pos_hbm, cot_hbm, fil_hbm, out_ref, wide_ref, fil_ref, lat_ref, pos_ref, sem):
    natom, width = cot_hbm.shape
    nk = lat_ref.shape[1]
    copies = [
        pltpu.make_async_copy(pos_hbm, pos_ref, sem.at[0]),
        pltpu.make_async_copy(lat_hbm, lat_ref, sem.at[1]),
        pltpu.make_async_copy(cot_hbm, out_ref.at[pl.ds(0, natom)], sem.at[2]),
        pltpu.make_async_copy(fil_hbm, fil_ref, sem.at[3]),
    ]
    for copy in copies:
        copy.start()
    copies[0].wait()
    x = pos_ref[...]
    hi = x.astype(bf16).astype(f32)
    rest = x - hi
    mid = rest.astype(bf16).astype(f32)
    low = rest - mid
    parts = jnp.concatenate([hi, mid, low], 0)
    rows = [parts[:, j * width : (j + 1) * width] for j in range(natom // width)]
    spare = out_ref.shape[0] - natom - 9 * len(rows)
    if spare:
        rows.append(jnp.zeros((spare, width), f32))
    out_ref[natom:, :] = jnp.concatenate(rows, 0).astype(bf16)
    copies[1].wait()
    row = lax.broadcasted_iota(jnp.int32, (nk, width), 0)
    col = lax.broadcasted_iota(jnp.int32, (nk, width), 1)
    spread = (row == col % nk).astype(bf16)
    lat = lat_ref[...].astype(f32).astype(bf16)
    wide = jnp.dot(lat, spread, preferred_element_type=f32)
    wide_ref[...] = jnp.concatenate([wide, wide, wide[:2]], 0)
    copies[2].wait()
    copies[3].wait()


def pack(keep, lattice, positions, cotangent, filters):
    natom, width = cotangent.shape
    rows = -(-9 * (natom // width) // 8) * 8
    outs = [shape((natom + rows, width), bf16), shape((8, width), f32), shape(filters.shape, f32)]
    if keep:
        outs = [pltpu.VMEM(v.shape, v.dtype) for v in outs]
    return pl.pallas_call(
        pack_body,
        out_shape=outs,
        in_specs=[pl.BlockSpec(memory_space=pl.ANY)] * 4,
        out_specs=full_spec(3),
        scratch_shapes=[
            pltpu.VMEM(lattice.shape, lattice.dtype),
            pltpu.VMEM(positions.shape, positions.dtype),
            pltpu.SemaphoreType.DMA((4,)),
        ],
    )(lattice, positions, cotangent, filters)


def join_body(own_ref, got_ref, out_ref):
    out_ref[0:8, :] = own_ref[...]
    out_ref[8:16, :] = got_ref[...]


def table_body(nk, lat_ref, out_ref):
    for h in range(2):
        out_ref[h * nk : (h + 1) * nk, :] = lat_ref[8 * h : 8 * (h + 1), :].T[0:nk]


def coordinates(block, natom):
    rows = block[natom:, :].astype(f32)
    chunks = natom // block.shape[1]
    out = []
    for d in range(3):
        pieces = []
        for j in range(chunks):
            at = [9 * j + 3 * p + d for p in range(3)]
            pieces.append((rows[at[0] : at[0] + 1] + rows[at[1] : at[1] + 1]) + rows[at[2] : at[2] + 1])
        out.append(jnp.concatenate(pieces, 1))
    return out


def factor_body(natom, nk, pairs, blocks, started, last, *refs):
    atoms = sorted({z for z, t in pairs})
    zb, refs = dict(zip(atoms, refs)), refs[len(atoms) :]
    tables, refs = dict(zip(blocks, refs)), refs[len(blocks) :]
    before, refs = (dict(zip(blocks, refs)), refs[len(blocks) :]) if started else ({}, refs)
    tiles, outs = dict(zip(pairs, refs)), refs[len(pairs) :]
    where = {z: coordinates(ref, natom) for z, ref in zb.items()}

    def phase(z, t, i):
        at = (t % 2) * nk + i
        cols = [tables[t][at : at + step, d : d + 1] for d in range(3)]
        return cols[0] * where[z][0] + cols[1] * where[z][1] + cols[2] * where[z][2]

    cot = {z: ref[0:natom, :] for z, ref in zb.items()}
    step = 32
    for b, t in enumerate(blocks):
        for i in range(0, nk, step):
            sums = [None, None]
            for z in atoms:
                for k, value in enumerate(cos_sin(phase(z, t, i))):
                    value = value.astype(bf16)
                    tiles[z, t][k * nk + i : k * nk + i + step, :] = value
                    part = jnp.dot(value, cot[z], preferred_element_type=f32)
                    sums[k] = part if sums[k] is None else sums[k] + part
            for k, total in enumerate(sums):
                row = k * nk + i
                if started:
                    total = total + before[t][row : row + step, :]
                if last:
                    outs[0][2 * nk * b + row : 2 * nk * b + row + step, :] = total.astype(outs[0].dtype)
                else:
                    outs[b][row : row + step, :] = total


def shuffled(ref, flip, half, nk):
    rows = [ref[2 * nk * (t ^ flip) : 2 * nk * ((t ^ flip) + 1), :] for t in range(half)]
    return jnp.concatenate(rows, 0).astype(f32)


def pair_body(own_ref, got_ref, f_ref, fb_ref):
    total = own_ref[...] + got_ref[...].astype(f32)
    f_ref[...] = total
    fb_ref[...] = total.astype(bf16)


def weight_body(half, nk, flips, scale, *refs):
    total = refs[0][...]
    for ref, flip in zip(refs[1:], flips):
        total = total + shuffled(ref, flip // 2, half, nk)
    total = total * scale
    fb = refs[1 + len(flips) : 1 + len(flips) + half]
    weight_ref, head_ref = refs[1 + len(flips) + half :]
    for t in range(half):
        fil = fb[t][...]
        rows = total[2 * nk * t : 2 * nk * (t + 1)] * jnp.concatenate([fil, fil], 0)
        weight_ref[:, 2 * nk * t : 2 * nk * (t + 1)] = rows.T.astype(bf16)
    head_ref[...] = total[0 : 2 * nk]


def part_of(weight_ref, tiles):
    tile = jnp.concatenate([ref[...] for ref in tiles], 0)
    return jnp.dot(weight_ref[...], tile, preferred_element_type=f32)


def mine_body(nz, half, weight_ref, *refs):
    for z in range(nz):
        refs[nz * half + z][...] = part_of(weight_ref, refs[z * half : (z + 1) * half])


def node_body(half, choices, *refs):
    weight_ref, refs = refs[0], refs[1:]
    out_ref = refs[-1]

    def one(part_ref, *tiles):
        total = part_ref[...] + part_of(weight_ref, tiles)
        out_ref[...] = total.T.astype(out_ref.dtype)

    groups = [refs[i * (half + 1) : (i + 1) * (half + 1)] for i in range(len(choices))]
    if len(choices) == 1:
        one(*groups[0])
        return
    plane = lax.axis_index("atoms")
    for planes, group in zip(choices, groups):
        taken = plane == planes[0]
        for other in planes[1:]:
            taken = taken | (plane == other)
        pl.when(taken)(lambda group=group: one(*group))


def own_body(half, head_ref, saved_ref, weight_ref, *refs):
    node_body(half, [None], weight_ref, *refs[:-1])
    grad_ref = refs[-1]
    nk = grad_ref.shape[0]
    grad_ref[...] = head_ref[0:nk] * saved_ref[0] + head_ref[nk : 2 * nk] * saved_ref[1]


def final_body(scale, *refs):
    total = refs[0][...]
    for ref in refs[1:-1]:
        total = total + ref[...].astype(f32)
    refs[-1][...] = (total * scale).astype(bf16)


def shape(dims, kind):
    return jax.ShapeDtypeStruct(dims, kind)


def local(lattice, positions, cotangent, filters, saved_factor):
    nz = lax.axis_size("atoms")
    nq = lax.axis_size("kvec")
    natom, width = cotangent.shape
    nk = lattice.shape[1]
    half = nq // 2
    count = half * nk
    scale_n = 1.0 / math.sqrt(natom * nz * nq)
    scale_k = 1.0 / math.sqrt(nk * nz * nq)
    keep = nz * natom * 4 * count * 2 <= VMEM_BUDGET

    def swap(value, flip):
        return lax.ppermute(value, "kvec", [(i, i ^ flip) for i in range(nq)])

    def send(value, targets):
        return lax.ppermute(value, "atoms", list(enumerate(targets)))

    def run(body, outs, *args, keep_args=keep, keep_outs=keep):
        return call(body, outs, *args, keep_args=keep_args, keep_outs=keep_outs)

    zbuf, wide, filters = pack(keep, lattice, positions, cotangent, filters)
    ring = gather_order(nz)
    flips = list(range(2, nq, 2))
    zb = {0: zbuf}
    for d in ring:
        zb[d] = send(zbuf, [(i - d) % nz for i in range(nz)])
    (cores,) = run(join_body, [shape((16, width), f32)], wide, swap(wide, 1))
    lats = [cores] + [swap(cores, s) for s in flips]
    fils = [filters] + [swap(filters, s) for s in flips]
    table = {}
    for s, lat in zip([0] + flips, lats):
        (both,) = run(lambda *refs: table_body(nk, *refs), [shape((2 * nk, 8), f32)], lat)
        table[s] = table[s + 1] = both
    mine = list(range(0, nq, 2))
    theirs = list(range(1, nq, 2))
    tiles = {}
    total = {}

    def factor(atoms, blocks, last=None):
        pairs = [(z, t) for z in sorted(atoms) for t in blocks]
        outs = [shape((2 * nk, natom), bf16)] * len(pairs)
        if last is None:
            outs += [shape((2 * nk, width), f32)] * len(blocks)
        else:
            outs.append(shape((2 * nk * len(blocks), width), last))
        started = blocks[0] in total
        args = [zb[z] for z in sorted(atoms)] + [table[t] for t in blocks] + [total[t] for t in blocks if started]
        body = lambda *refs: factor_body(natom, nk, pairs, blocks, started, last is not None, *refs)
        got = run(body, outs, *args)
        tiles.update(zip(pairs, got))
        if last is None:
            total.update(zip(blocks, got[len(pairs) :]))
        return got[-1]

    order = [0] + ring
    cut = max(1, len(order) - 2)
    early = order[: min(2, cut)]
    for z in early:
        factor([z], [0, 1])
    for t in flips:
        factor(early, [t, t + 1])
    for z in order[len(early) : cut]:
        factor([z], list(range(nq)))
    sent = factor(order[cut:], theirs, bf16)
    kept = factor(order[cut:], mine, f32)
    pair, pair16 = run(
        pair_body,
        [shape((2 * count, width), f32), shape((2 * count, width), bf16)],
        kept,
        swap(sent, 1),
    )
    got = [swap(pair16, s) for s in flips]
    weight, head = run(
        lambda *refs: weight_body(half, nk, flips, scale_n, *refs),
        [shape((width, 2 * count), bf16), shape((2 * nk, width), f32)],
        pair,
        *got,
        *fils,
    )
    other = swap(weight, 1)
    parts = run(
        lambda *refs: mine_body(nz, half, *refs),
        [shape((width, natom), f32)] * nz,
        weight,
        *[tiles[s, t] for s in order for t in mine],
    )
    parts = dict(zip(order, parts))
    landed = []
    for targets in reduce_rounds(nz):
        planes = {}
        for i, target in enumerate(targets):
            planes.setdefault((target - i) % nz, []).append(i)
        (node,) = run(
            lambda *refs: node_body(half, list(planes.values()), *refs),
            [shape((natom, width), bf16)],
            other,
            *[v for d in planes for v in [parts[d], *[tiles[d, t] for t in theirs]]],
        )
        landed.append(send(node, targets))
    own, filter_grad = run(
        lambda *refs: own_body(half, *refs),
        [shape((natom, width), f32), shape((nk, width), f32)],
        head,
        saved_factor,
        other,
        parts[0],
        *[tiles[0, t] for t in theirs],
    )
    (node_grad,) = run(
        lambda *refs: final_body(scale_k, *refs),
        [shape((natom, width), bf16)],
        own,
        *landed,
        keep_outs=False,
    )
    return (node_grad, filter_grad)


def gather_order(nz):
    return list(range(nz - 1, 0, -1))


def reduce_rounds(nz):
    ring = list(range(nz))
    if nz <= 4:
        ring = ring[:1] + ring[1::2] + ring[2::2][::-1]
    place = {z: i for i, z in enumerate(ring)}
    return [[ring[(place[z] + by) % nz] for z in range(nz)] for by in range(1, nz)]


def solution(mesh):
    in_specs = (
        P(None, ("atoms", "kvec")),
        P(None, ("beads", "atoms", "kvec")),
        P(("beads", "atoms", "kvec"), None),
        P(("atoms", "kvec"), None),
        P(None, ("beads", "atoms", "kvec"), None),
    )
    out_specs = (P(("beads", "atoms", "kvec"), None), P(("beads", "atoms", "kvec"), None))
    return jax.shard_map(local, mesh=mesh, in_specs=in_specs, out_specs=out_specs, check_vma=False)
```

```python
import math

import jax
import jax.numpy as jnp
from jax import lax
from jax.experimental import pallas as pl
from jax.experimental.pallas import tpu as pltpu
from jax.sharding import PartitionSpec as P


f32 = jnp.float32
bf16 = jnp.bfloat16


SIN_COEF = None
COS_COEF = None


def _fit():
    import numpy as np

    n = 4001
    t = np.cos(np.pi * (np.arange(n) + 0.5) / n)
    u = (t + 1.0) * 0.125
    r = np.sqrt(u)
    root = math.sqrt(2.0)
    sin_ratio = np.where(r > 1e-9, root * np.sin(np.pi * r) / np.maximum(r, 1e-9), root * np.pi)
    cheb = np.polynomial.chebyshev.Chebyshev
    s = cheb.fit(u, sin_ratio, 4, domain=[0.0, 0.25]).convert(kind=np.polynomial.Polynomial)
    c = cheb.fit(u, root * np.cos(np.pi * r), 4, domain=[0.0, 0.25]).convert(kind=np.polynomial.Polynomial)
    return tuple(float(v) for v in s.coef), tuple(float(v) for v in c.coef)


SIN_COEF, COS_COEF = _fit()


def _horner(coef, u):
    acc = jnp.full_like(u, coef[-1])
    for value in coef[-2::-1]:
        acc = acc * u + value
    return acc


def cos_sin(phase):
    r = phase - jnp.round(phase)
    u = r * r
    s = r * _horner(SIN_COEF, u)
    c = _horner(COS_COEF, u)
    return 1.0 - s * s, s * c


def full_spec(count):
    return [pl.BlockSpec(memory_space=pltpu.VMEM)] * count


VMEM_BUDGET = 4 * 1024 * 1024
PIECES = 4


def call(body, outs, *args, keep_args=True, keep_outs=True):
    if keep_args:
        args = [pltpu.with_memory_space_constraint(arg, pltpu.VMEM) for arg in args]
    if keep_outs:
        outs = [pltpu.VMEM(v.shape, v.dtype) for v in outs]
    return pl.pallas_call(
        body,
        out_shape=outs,
        in_specs=full_spec(len(args)),
        out_specs=full_spec(len(outs)),
    )(*args)


def pack_body(lat_hbm, pos_hbm, cot_hbm, fil_hbm, out_ref, wide_ref, fil_ref, lat_ref, pos_ref, sem):
    natom, width = cot_hbm.shape
    nk = lat_ref.shape[1]
    copies = [
        pltpu.make_async_copy(pos_hbm, pos_ref, sem.at[0]),
        pltpu.make_async_copy(lat_hbm, lat_ref, sem.at[1]),
        pltpu.make_async_copy(fil_hbm, fil_ref, sem.at[2]),
    ]
    piece = natom // PIECES
    for j in range(PIECES):
        rows = pl.ds(j * piece, piece)
        copies.append(pltpu.make_async_copy(cot_hbm.at[rows], out_ref.at[rows], sem.at[3 + j]))
    for copy in copies:
        copy.start()
    copies[0].wait()
    x = pos_ref[...]
    hi = x.astype(bf16).astype(f32)
    rest = x - hi
    mid = rest.astype(bf16).astype(f32)
    low = rest - mid
    parts = jnp.concatenate([hi, mid, low], 0)
    rows = [parts[:, j * width : (j + 1) * width] for j in range(natom // width)]
    spare = out_ref.shape[0] - natom - 9 * len(rows)
    if spare:
        rows.append(jnp.zeros((spare, width), f32))
    out_ref[natom:, :] = jnp.concatenate(rows, 0).astype(bf16)
    copies[1].wait()
    row = lax.broadcasted_iota(jnp.int32, (nk, width), 0)
    col = lax.broadcasted_iota(jnp.int32, (nk, width), 1)
    spread = (row == col % nk).astype(bf16)
    lat = lat_ref[...].astype(f32).astype(bf16)
    wide = jnp.dot(lat, spread, preferred_element_type=f32)
    wide_ref[...] = jnp.concatenate([wide, wide, wide[:2]], 0)
    for copy in copies[2:]:
        copy.wait()


def pack(keep, lattice, positions, cotangent, filters):
    natom, width = cotangent.shape
    rows = -(-9 * (natom // width) // 8) * 8
    outs = [shape((natom + rows, width), bf16), shape((8, width), f32), shape(filters.shape, f32)]
    if keep:
        outs = [pltpu.VMEM(v.shape, v.dtype) for v in outs]
    return pl.pallas_call(
        pack_body,
        out_shape=outs,
        in_specs=[pl.BlockSpec(memory_space=pl.ANY)] * 4,
        out_specs=full_spec(3),
        scratch_shapes=[
            pltpu.VMEM(lattice.shape, lattice.dtype),
            pltpu.VMEM(positions.shape, positions.dtype),
            pltpu.SemaphoreType.DMA((3 + PIECES,)),
        ],
    )(lattice, positions, cotangent, filters)


def join_body(own_ref, got_ref, out_ref):
    out_ref[0:8, :] = own_ref[...]
    out_ref[8:16, :] = got_ref[...]


def table_body(nk, lat_ref, out_ref):
    for h in range(2):
        out_ref[h * nk : (h + 1) * nk, :] = lat_ref[8 * h : 8 * (h + 1), :].T[0:nk]


def coordinates(block, natom):
    rows = block[natom:, :].astype(f32)
    chunks = natom // block.shape[1]
    out = []
    for d in range(3):
        pieces = []
        for j in range(chunks):
            at = [9 * j + 3 * p + d for p in range(3)]
            pieces.append((rows[at[0] : at[0] + 1] + rows[at[1] : at[1] + 1]) + rows[at[2] : at[2] + 1])
        out.append(jnp.concatenate(pieces, 1))
    return out


def factor_body(natom, nk, pairs, blocks, started, last, *refs):
    atoms = sorted({z for z, t in pairs})
    zb, refs = dict(zip(atoms, refs)), refs[len(atoms) :]
    tables, refs = dict(zip(blocks, refs)), refs[len(blocks) :]
    before, refs = (dict(zip(blocks, refs)), refs[len(blocks) :]) if started else ({}, refs)
    tiles, outs = dict(zip(pairs, refs)), refs[len(pairs) :]
    where = {z: coordinates(ref, natom) for z, ref in zb.items()}

    def phase(z, t, i):
        at = (t % 2) * nk + i
        cols = [tables[t][at : at + step, d : d + 1] for d in range(3)]
        return cols[0] * where[z][0] + cols[1] * where[z][1] + cols[2] * where[z][2]

    cot = {z: ref[0:natom, :] for z, ref in zb.items()}
    step = 32
    for b, t in enumerate(blocks):
        for i in range(0, nk, step):
            sums = [None, None]
            for z in atoms:
                for k, value in enumerate(cos_sin(phase(z, t, i))):
                    value = value.astype(bf16)
                    tiles[z, t][k * nk + i : k * nk + i + step, :] = value
                    part = jnp.dot(value, cot[z], preferred_element_type=f32)
                    sums[k] = part if sums[k] is None else sums[k] + part
            for k, total in enumerate(sums):
                row = k * nk + i
                if started:
                    total = total + before[t][row : row + step, :]
                if last:
                    outs[0][2 * nk * b + row : 2 * nk * b + row + step, :] = total.astype(outs[0].dtype)
                else:
                    outs[b][row : row + step, :] = total


def shuffled(ref, flip, half, nk):
    rows = [ref[2 * nk * (t ^ flip) : 2 * nk * ((t ^ flip) + 1), :] for t in range(half)]
    return jnp.concatenate(rows, 0).astype(f32)


def pair_body(own_ref, got_ref, f_ref, fb_ref):
    total = own_ref[...] + got_ref[...].astype(f32)
    f_ref[...] = total
    fb_ref[...] = total.astype(bf16)


def weight_body(half, nk, flips, scale, *refs):
    total = refs[0][...]
    for ref, flip in zip(refs[1:], flips):
        total = total + shuffled(ref, flip // 2, half, nk)
    total = total * scale
    fb = refs[1 + len(flips) : 1 + len(flips) + half]
    weight_ref, head_ref = refs[1 + len(flips) + half :]
    for t in range(half):
        fil = fb[t][...]
        rows = total[2 * nk * t : 2 * nk * (t + 1)] * jnp.concatenate([fil, fil], 0)
        weight_ref[:, 2 * nk * t : 2 * nk * (t + 1)] = rows.T.astype(bf16)
    head_ref[...] = total[0 : 2 * nk]


def part_of(weight_ref, tiles):
    tile = jnp.concatenate([ref[...] for ref in tiles], 0)
    return jnp.dot(weight_ref[...], tile, preferred_element_type=f32)


def mine_body(nz, half, weight_ref, *refs):
    for z in range(nz):
        refs[nz * half + z][...] = part_of(weight_ref, refs[z * half : (z + 1) * half])


def node_body(half, choices, *refs):
    weight_ref, refs = refs[0], refs[1:]
    out_ref = refs[-1]

    def one(part_ref, *tiles):
        total = part_ref[...] + part_of(weight_ref, tiles)
        out_ref[...] = total.astype(out_ref.dtype)

    groups = [refs[i * (half + 1) : (i + 1) * (half + 1)] for i in range(len(choices))]
    if len(choices) == 1:
        one(*groups[0])
        return
    plane = lax.axis_index("atoms")
    for planes, group in zip(choices, groups):
        taken = plane == planes[0]
        for other in planes[1:]:
            taken = taken | (plane == other)
        pl.when(taken)(lambda group=group: one(*group))


def own_body(half, head_ref, saved_ref, weight_ref, *refs):
    node_body(half, [None], weight_ref, *refs[:-1])
    grad_ref = refs[-1]
    nk = grad_ref.shape[0]
    grad_ref[...] = head_ref[0:nk] * saved_ref[0] + head_ref[nk : 2 * nk] * saved_ref[1]


def final_body(scale, *refs):
    total = refs[0][...]
    for ref in refs[1:-1]:
        total = total + ref[...].astype(f32)
    refs[-1][...] = (total * scale).T.astype(bf16)


def shape(dims, kind):
    return jax.ShapeDtypeStruct(dims, kind)


def local(lattice, positions, cotangent, filters, saved_factor):
    nz = lax.axis_size("atoms")
    nq = lax.axis_size("kvec")
    natom, width = cotangent.shape
    nk = lattice.shape[1]
    half = nq // 2
    count = half * nk
    scale_n = 1.0 / math.sqrt(natom * nz * nq)
    scale_k = 1.0 / math.sqrt(nk * nz * nq)
    keep = nz * natom * 4 * count * 2 <= VMEM_BUDGET

    def swap(value, flip):
        return lax.ppermute(value, "kvec", [(i, i ^ flip) for i in range(nq)])

    def send(value, targets):
        return lax.ppermute(value, "atoms", list(enumerate(targets)))

    def run(body, outs, *args, keep_args=keep, keep_outs=keep):
        return call(body, outs, *args, keep_args=keep_args, keep_outs=keep_outs)

    zbuf, wide, filters = pack(keep, lattice, positions, cotangent, filters)
    ring = gather_order(nz)
    flips = list(range(2, nq, 2))
    zb = {0: zbuf}
    for d in ring:
        zb[d] = send(zbuf, [(i - d) % nz for i in range(nz)])
    (cores,) = run(join_body, [shape((16, width), f32)], wide, swap(wide, 1))
    lats = [cores] + [swap(cores, s) for s in flips]
    fils = [filters] + [swap(filters, s) for s in flips]
    table = {}
    for s, lat in zip([0] + flips, lats):
        (both,) = run(lambda *refs: table_body(nk, *refs), [shape((2 * nk, 8), f32)], lat)
        table[s] = table[s + 1] = both
    mine = list(range(0, nq, 2))
    theirs = list(range(1, nq, 2))
    tiles = {}
    total = {}

    def factor(atoms, blocks, last=None):
        pairs = [(z, t) for z in sorted(atoms) for t in blocks]
        outs = [shape((2 * nk, natom), bf16)] * len(pairs)
        if last is None:
            outs += [shape((2 * nk, width), f32)] * len(blocks)
        else:
            outs.append(shape((2 * nk * len(blocks), width), last))
        started = blocks[0] in total
        args = [zb[z] for z in sorted(atoms)] + [table[t] for t in blocks] + [total[t] for t in blocks if started]
        body = lambda *refs: factor_body(natom, nk, pairs, blocks, started, last is not None, *refs)
        got = run(body, outs, *args)
        tiles.update(zip(pairs, got))
        if last is None:
            total.update(zip(blocks, got[len(pairs) :]))
        return got[-1]

    order = [0] + ring
    cut = max(1, len(order) - 2)
    early = order[: min(2, cut)]
    for z in early:
        factor([z], [0, 1])
    for t in flips:
        factor(early, [t, t + 1])
    for z in order[len(early) : cut]:
        factor([z], list(range(nq)))
    sent = factor(order[cut:], theirs, bf16)
    kept = factor(order[cut:], mine, f32)
    pair, pair16 = run(
        pair_body,
        [shape((2 * count, width), f32), shape((2 * count, width), bf16)],
        kept,
        swap(sent, 1),
    )
    got = [swap(pair16, s) for s in flips]
    weight, head = run(
        lambda *refs: weight_body(half, nk, flips, scale_n, *refs),
        [shape((width, 2 * count), bf16), shape((2 * nk, width), f32)],
        pair,
        *got,
        *fils,
    )
    other = swap(weight, 1)
    parts = run(
        lambda *refs: mine_body(nz, half, *refs),
        [shape((width, natom), f32)] * nz,
        weight,
        *[tiles[s, t] for s in order for t in mine],
    )
    parts = dict(zip(order, parts))
    landed = []
    for targets in reduce_rounds(nz):
        planes = {}
        for i, target in enumerate(targets):
            planes.setdefault((target - i) % nz, []).append(i)
        (node,) = run(
            lambda *refs: node_body(half, list(planes.values()), *refs),
            [shape((width, natom), bf16)],
            other,
            *[v for d in planes for v in [parts[d], *[tiles[d, t] for t in theirs]]],
        )
        landed.append(send(node, targets))
    own, filter_grad = run(
        lambda *refs: own_body(half, *refs),
        [shape((width, natom), f32), shape((nk, width), f32)],
        head,
        saved_factor,
        other,
        parts[0],
        *[tiles[0, t] for t in theirs],
    )
    (node_grad,) = run(
        lambda *refs: final_body(scale_k, *refs),
        [shape((natom, width), bf16)],
        own,
        *landed,
        keep_outs=False,
    )
    return (node_grad, filter_grad)


def gather_order(nz):
    return list(range(nz - 1, 0, -1))


def reduce_rounds(nz):
    ring = list(range(nz))
    if nz <= 4:
        ring = ring[:1] + ring[1::2] + ring[2::2][::-1]
    place = {z: i for i, z in enumerate(ring)}
    return [[ring[(place[z] + by) % nz] for z in range(nz)] for by in range(1, nz)]


def solution(mesh):
    in_specs = (
        P(None, ("atoms", "kvec")),
        P(None, ("beads", "atoms", "kvec")),
        P(("beads", "atoms", "kvec"), None),
        P(("atoms", "kvec"), None),
        P(None, ("beads", "atoms", "kvec"), None),
    )
    out_specs = (P(("beads", "atoms", "kvec"), None), P(("beads", "atoms", "kvec"), None))
    return jax.shard_map(local, mesh=mesh, in_specs=in_specs, out_specs=out_specs, check_vma=False)
```

```python
import math

import jax
import jax.numpy as jnp
from jax import lax
from jax.experimental import pallas as pl
from jax.experimental.pallas import tpu as pltpu
from jax.sharding import PartitionSpec as P


f32 = jnp.float32
bf16 = jnp.bfloat16


SIN_COEF = None
COS_COEF = None


def _fit():
    import numpy as np

    n = 4001
    t = np.cos(np.pi * (np.arange(n) + 0.5) / n)
    u = (t + 1.0) * 0.125
    r = np.sqrt(u)
    root = math.sqrt(2.0)
    sin_ratio = np.where(r > 1e-9, root * np.sin(np.pi * r) / np.maximum(r, 1e-9), root * np.pi)
    cheb = np.polynomial.chebyshev.Chebyshev
    s = cheb.fit(u, sin_ratio, 4, domain=[0.0, 0.25]).convert(kind=np.polynomial.Polynomial)
    c = cheb.fit(u, root * np.cos(np.pi * r), 4, domain=[0.0, 0.25]).convert(kind=np.polynomial.Polynomial)
    return tuple(float(v) for v in s.coef), tuple(float(v) for v in c.coef)


SIN_COEF, COS_COEF = _fit()


def _horner(coef, u):
    acc = jnp.full_like(u, coef[-1])
    for value in coef[-2::-1]:
        acc = acc * u + value
    return acc


def cos_sin(phase):
    r = phase - jnp.round(phase)
    u = r * r
    s = r * _horner(SIN_COEF, u)
    c = _horner(COS_COEF, u)
    return 1.0 - s * s, s * c


def full_spec(count):
    return [pl.BlockSpec(memory_space=pltpu.VMEM)] * count


VMEM_BUDGET = 4 * 1024 * 1024
PIECES = 4


def call(body, outs, *args, keep_args=True, keep_outs=True):
    if keep_args:
        args = [pltpu.with_memory_space_constraint(arg, pltpu.VMEM) for arg in args]
    if keep_outs:
        outs = [pltpu.VMEM(v.shape, v.dtype) for v in outs]
    return pl.pallas_call(
        body,
        out_shape=outs,
        in_specs=full_spec(len(args)),
        out_specs=full_spec(len(outs)),
    )(*args)


def pack_body(lat_hbm, pos_hbm, cot_hbm, fil_hbm, out_ref, wide_ref, fil_ref, lat_ref, pos_ref, sem):
    natom, width = cot_hbm.shape
    nk = lat_ref.shape[1]
    copies = [
        pltpu.make_async_copy(pos_hbm, pos_ref, sem.at[0]),
        pltpu.make_async_copy(lat_hbm, lat_ref, sem.at[1]),
        pltpu.make_async_copy(fil_hbm, fil_ref, sem.at[2]),
    ]
    piece = natom // PIECES
    for j in range(PIECES):
        rows = pl.ds(j * piece, piece)
        copies.append(pltpu.make_async_copy(cot_hbm.at[rows], out_ref.at[rows], sem.at[3 + j]))
    for copy in copies:
        copy.start()
    copies[0].wait()
    x = pos_ref[...]
    hi = x.astype(bf16).astype(f32)
    rest = x - hi
    mid = rest.astype(bf16).astype(f32)
    low = rest - mid
    parts = jnp.concatenate([hi, mid, low], 0)
    rows = [parts[:, j * width : (j + 1) * width] for j in range(natom // width)]
    spare = out_ref.shape[0] - natom - 9 * len(rows)
    if spare:
        rows.append(jnp.zeros((spare, width), f32))
    out_ref[natom:, :] = jnp.concatenate(rows, 0).astype(bf16)
    copies[1].wait()
    row = lax.broadcasted_iota(jnp.int32, (nk, width), 0)
    col = lax.broadcasted_iota(jnp.int32, (nk, width), 1)
    spread = (row == col % nk).astype(bf16)
    lat = lat_ref[...].astype(f32).astype(bf16)
    wide = jnp.dot(lat, spread, preferred_element_type=f32)
    wide_ref[...] = jnp.concatenate([wide, wide, wide[:2]], 0)
    for copy in copies[2:]:
        copy.wait()


def pack(keep, lattice, positions, cotangent, filters):
    natom, width = cotangent.shape
    rows = -(-9 * (natom // width) // 8) * 8
    outs = [shape((natom + rows, width), bf16), shape((8, width), f32), shape(filters.shape, f32)]
    if keep:
        outs = [pltpu.VMEM(v.shape, v.dtype) for v in outs]
    return pl.pallas_call(
        pack_body,
        out_shape=outs,
        in_specs=[pl.BlockSpec(memory_space=pl.ANY)] * 4,
        out_specs=full_spec(3),
        scratch_shapes=[
            pltpu.VMEM(lattice.shape, lattice.dtype),
            pltpu.VMEM(positions.shape, positions.dtype),
            pltpu.SemaphoreType.DMA((3 + PIECES,)),
        ],
    )(lattice, positions, cotangent, filters)


def join_body(own_ref, got_ref, out_ref):
    out_ref[0:8, :] = own_ref[...]
    out_ref[8:16, :] = got_ref[...]


def table_body(nk, lat_ref, out_ref):
    for h in range(2):
        out_ref[h * nk : (h + 1) * nk, :] = lat_ref[8 * h : 8 * (h + 1), :].T[0:nk]


def coordinates(block, natom):
    rows = block[natom:, :].astype(f32)
    chunks = natom // block.shape[1]
    out = []
    for d in range(3):
        pieces = []
        for j in range(chunks):
            at = [9 * j + 3 * p + d for p in range(3)]
            pieces.append((rows[at[0] : at[0] + 1] + rows[at[1] : at[1] + 1]) + rows[at[2] : at[2] + 1])
        out.append(jnp.concatenate(pieces, 1))
    return out


def factor_body(natom, nk, pairs, blocks, started, last, *refs):
    atoms = sorted({z for z, t in pairs})
    zb, refs = dict(zip(atoms, refs)), refs[len(atoms) :]
    tables, refs = dict(zip(blocks, refs)), refs[len(blocks) :]
    before, refs = (dict(zip(blocks, refs)), refs[len(blocks) :]) if started else ({}, refs)
    tiles, outs = dict(zip(pairs, refs)), refs[len(pairs) :]
    where = {z: coordinates(ref, natom) for z, ref in zb.items()}

    def phase(z, t, i):
        at = (t % 2) * nk + i
        cols = [tables[t][at : at + step, d : d + 1] for d in range(3)]
        return cols[0] * where[z][0] + cols[1] * where[z][1] + cols[2] * where[z][2]

    cot = {z: ref[0:natom, :] for z, ref in zb.items()}
    step = 32
    for b, t in enumerate(blocks):
        for i in range(0, nk, step):
            sums = [None, None]
            for z in atoms:
                for k, value in enumerate(cos_sin(phase(z, t, i))):
                    value = value.astype(bf16)
                    tiles[z, t][k * nk + i : k * nk + i + step, :] = value
                    part = jnp.dot(value, cot[z], preferred_element_type=f32)
                    sums[k] = part if sums[k] is None else sums[k] + part
            for k, total in enumerate(sums):
                row = k * nk + i
                if started:
                    total = total + before[t][row : row + step, :]
                if last:
                    for out in outs:
                        out[2 * nk * b + row : 2 * nk * b + row + step, :] = total.astype(out.dtype)
                else:
                    outs[b][row : row + step, :] = total


def shuffled(ref, flip, nq, nk):
    rows = [ref[2 * nk * (t ^ flip) : 2 * nk * ((t ^ flip) + 1), :] for t in range(nq)]
    return jnp.concatenate(rows, 0).astype(f32)


def pair_body(nq, nk, flips, own_ref, *refs):
    total = own_ref[...]
    for ref, flip in zip(refs, flips):
        total = total + shuffled(ref, flip, nq, nk)
    for out in refs[len(flips) :]:
        out[...] = total.astype(out.dtype)


def weight_body(nq, nk, scale, own_ref, got_ref, *refs):
    total = (own_ref[...] + shuffled(got_ref, 1, nq, nk)) * scale
    weight_ref, head_ref = refs[nq:]
    for t in range(nq):
        fil = refs[t][...]
        rows = total[2 * nk * t : 2 * nk * (t + 1)] * jnp.concatenate([fil, fil], 0)
        weight_ref[:, 2 * nk * t : 2 * nk * (t + 1)] = rows.T.astype(bf16)
    head_ref[...] = total[0 : 2 * nk]


def part_of(weight_ref, tiles):
    tile = jnp.concatenate([ref[...] for ref in tiles], 0)
    return jnp.dot(weight_ref[...], tile, preferred_element_type=f32)


def node_body(nq, choices, weight_ref, *refs):
    out_ref = refs[-1]

    def one(*tiles):
        out_ref[...] = part_of(weight_ref, tiles).astype(out_ref.dtype)

    groups = [refs[i * nq : (i + 1) * nq] for i in range(len(choices))]
    if len(choices) == 1:
        one(*groups[0])
        return
    plane = lax.axis_index("atoms")
    for planes, group in zip(choices, groups):
        taken = plane == planes[0]
        for other in planes[1:]:
            taken = taken | (plane == other)
        pl.when(taken)(lambda group=group: one(*group))


def own_body(nq, head_ref, saved_ref, weight_ref, *refs):
    node_body(nq, [None], weight_ref, *refs[:-1])
    grad_ref = refs[-1]
    nk = grad_ref.shape[0]
    grad_ref[...] = head_ref[0:nk] * saved_ref[0] + head_ref[nk : 2 * nk] * saved_ref[1]


def final_body(scale, *refs):
    total = refs[0][...]
    for ref in refs[1:-1]:
        total = total + ref[...].astype(f32)
    refs[-1][...] = (total * scale).T.astype(bf16)


def shape(dims, kind):
    return jax.ShapeDtypeStruct(dims, kind)


def local(lattice, positions, cotangent, filters, saved_factor):
    nz = lax.axis_size("atoms")
    nq = lax.axis_size("kvec")
    natom, width = cotangent.shape
    nk = lattice.shape[1]
    scale_n = 1.0 / math.sqrt(natom * nz * nq)
    scale_k = 1.0 / math.sqrt(nk * nz * nq)
    keep = nz * natom * 2 * nk * nq * 2 <= VMEM_BUDGET

    def swap(value, flip):
        return lax.ppermute(value, "kvec", [(i, i ^ flip) for i in range(nq)])

    def send(value, targets):
        return lax.ppermute(value, "atoms", list(enumerate(targets)))

    def run(body, outs, *args, keep_args=keep, keep_outs=keep):
        return call(body, outs, *args, keep_args=keep_args, keep_outs=keep_outs)

    zbuf, wide, filters = pack(keep, lattice, positions, cotangent, filters)
    ring = gather_order(nz)
    flips = list(range(2, nq, 2))
    zb = {0: zbuf}
    for d in ring:
        zb[d] = send(zbuf, [(i - d) % nz for i in range(nz)])
    (cores,) = run(join_body, [shape((16, width), f32)], wide, swap(wide, 1))
    lats = [cores] + [swap(cores, s) for s in flips]
    fils = [filters] + [swap(filters, s) for s in flips]
    fils = [f for near in fils for f in (near, swap(near, 1))]
    table = {}
    for s, lat in zip([0] + flips, lats):
        (both,) = run(lambda *refs: table_body(nk, *refs), [shape((2 * nk, 8), f32)], lat)
        table[s] = table[s + 1] = both
    tiles = {}
    total = {}

    def factor(atoms, blocks, last=False):
        pairs = [(z, t) for z in sorted(atoms) for t in blocks]
        outs = [shape((2 * nk, natom), bf16)] * len(pairs)
        if last:
            outs += [shape((2 * nk * len(blocks), width), kind) for kind in (f32, bf16)]
        else:
            outs += [shape((2 * nk, width), f32)] * len(blocks)
        started = blocks[0] in total
        args = [zb[z] for z in sorted(atoms)] + [table[t] for t in blocks] + [total[t] for t in blocks if started]
        body = lambda *refs: factor_body(natom, nk, pairs, blocks, started, last, *refs)
        got = run(body, outs, *args)
        tiles.update(zip(pairs, got))
        total.update(zip(blocks, got[len(pairs) :]))
        return got[len(pairs) :]

    order = [0] + ring
    cut = max(1, len(order) - 2)
    early = order[: min(2, cut)]
    for z in early:
        factor([z], [0, 1])
    for t in flips:
        factor(early, [t, t + 1])
    for z in order[len(early) : cut]:
        factor([z], list(range(nq)))
    kept, sent = factor(order[cut:], list(range(nq)), last=True)
    dims = (2 * nk * nq, width)
    pair, pair16 = run(
        lambda *refs: pair_body(nq, nk, flips, *refs),
        [shape(dims, f32), shape(dims, bf16)],
        kept,
        *[swap(sent, s) for s in flips],
    )
    weight, head = run(
        lambda *refs: weight_body(nq, nk, scale_n, *refs),
        [shape((width, 2 * nk * nq), bf16), shape((2 * nk, width), f32)],
        pair,
        swap(pair16, 1),
        *fils,
    )
    landed = []
    for targets in reduce_rounds(nz):
        planes = {}
        for i, target in enumerate(targets):
            planes.setdefault((target - i) % nz, []).append(i)
        (node,) = run(
            lambda *refs: node_body(nq, list(planes.values()), *refs),
            [shape((width, natom), bf16)],
            weight,
            *[tiles[d, t] for d in planes for t in range(nq)],
        )
        landed.append(send(node, targets))
    own, filter_grad = run(
        lambda *refs: own_body(nq, *refs),
        [shape((width, natom), f32), shape((nk, width), f32)],
        head,
        saved_factor,
        weight,
        *[tiles[0, t] for t in range(nq)],
    )
    (node_grad,) = run(
        lambda *refs: final_body(scale_k, *refs),
        [shape((natom, width), bf16)],
        own,
        *landed,
        keep_outs=False,
    )
    return (node_grad, filter_grad)


def gather_order(nz):
    return list(range(nz - 1, 0, -1))


def reduce_rounds(nz):
    ring = list(range(nz))
    if nz <= 4:
        ring = ring[:1] + ring[1::2] + ring[2::2][::-1]
    place = {z: i for i, z in enumerate(ring)}
    return [[ring[(place[z] + by) % nz] for z in range(nz)] for by in range(1, nz)]


def solution(mesh):
    in_specs = (
        P(None, ("atoms", "kvec")),
        P(None, ("beads", "atoms", "kvec")),
        P(("beads", "atoms", "kvec"), None),
        P(("atoms", "kvec"), None),
        P(None, ("beads", "atoms", "kvec"), None),
    )
    out_specs = (P(("beads", "atoms", "kvec"), None), P(("beads", "atoms", "kvec"), None))
    return jax.shard_map(local, mesh=mesh, in_specs=in_specs, out_specs=out_specs, check_vma=False)
```

```python
import math

import jax
import jax.numpy as jnp
from jax import lax
from jax.experimental import pallas as pl
from jax.experimental.pallas import tpu as pltpu
from jax.sharding import PartitionSpec as P


f32 = jnp.float32
bf16 = jnp.bfloat16


SIN_COEF = None
COS_COEF = None


def _fit():
    import numpy as np

    n = 4001
    t = np.cos(np.pi * (np.arange(n) + 0.5) / n)
    u = (t + 1.0) * 0.125
    r = np.sqrt(u)
    root = math.sqrt(2.0)
    sin_ratio = np.where(r > 1e-9, root * np.sin(np.pi * r) / np.maximum(r, 1e-9), root * np.pi)
    cheb = np.polynomial.chebyshev.Chebyshev
    s = cheb.fit(u, sin_ratio, 4, domain=[0.0, 0.25]).convert(kind=np.polynomial.Polynomial)
    c = cheb.fit(u, root * np.cos(np.pi * r), 4, domain=[0.0, 0.25]).convert(kind=np.polynomial.Polynomial)
    return tuple(float(v) for v in s.coef), tuple(float(v) for v in c.coef)


SIN_COEF, COS_COEF = _fit()


def _horner(coef, u):
    acc = jnp.full_like(u, coef[-1])
    for value in coef[-2::-1]:
        acc = acc * u + value
    return acc


def cos_sin(phase):
    r = phase - jnp.round(phase)
    u = r * r
    s = r * _horner(SIN_COEF, u)
    c = _horner(COS_COEF, u)
    return 1.0 - s * s, s * c


def full_spec(count):
    return [pl.BlockSpec(memory_space=pltpu.VMEM)] * count


VMEM_BUDGET = 4 * 1024 * 1024
PIECES = 4


def call(body, outs, *args, keep_args=True, keep_outs=True):
    if keep_args:
        args = [pltpu.with_memory_space_constraint(arg, pltpu.VMEM) for arg in args]
    if keep_outs:
        outs = [pltpu.VMEM(v.shape, v.dtype) for v in outs]
    return pl.pallas_call(
        body,
        out_shape=outs,
        in_specs=full_spec(len(args)),
        out_specs=full_spec(len(outs)),
    )(*args)


def pack_body(lat_hbm, pos_hbm, cot_hbm, fil_hbm, out_ref, wide_ref, fil_ref, lat_ref, pos_ref, sem):
    natom, width = cot_hbm.shape
    nk = lat_ref.shape[1]
    copies = [
        pltpu.make_async_copy(pos_hbm, pos_ref, sem.at[0]),
        pltpu.make_async_copy(lat_hbm, lat_ref, sem.at[1]),
        pltpu.make_async_copy(fil_hbm, fil_ref, sem.at[2]),
    ]
    piece = natom // PIECES
    for j in range(PIECES):
        rows = pl.ds(j * piece, piece)
        copies.append(pltpu.make_async_copy(cot_hbm.at[rows], out_ref.at[rows], sem.at[3 + j]))
    for copy in copies:
        copy.start()
    copies[0].wait()
    x = pos_ref[...]
    hi = x.astype(bf16).astype(f32)
    rest = x - hi
    mid = rest.astype(bf16).astype(f32)
    low = rest - mid
    parts = jnp.concatenate([hi, mid, low], 0)
    rows = [parts[:, j * width : (j + 1) * width] for j in range(natom // width)]
    spare = out_ref.shape[0] - natom - 9 * len(rows)
    if spare:
        rows.append(jnp.zeros((spare, width), f32))
    out_ref[natom:, :] = jnp.concatenate(rows, 0).astype(bf16)
    copies[1].wait()
    row = lax.broadcasted_iota(jnp.int32, (nk, width), 0)
    col = lax.broadcasted_iota(jnp.int32, (nk, width), 1)
    spread = (row == col % nk).astype(bf16)
    lat = lat_ref[...].astype(f32).astype(bf16)
    wide = jnp.dot(lat, spread, preferred_element_type=f32)
    wide_ref[...] = jnp.concatenate([wide, wide, wide[:2]], 0)
    for copy in copies[2:]:
        copy.wait()


def pack(keep, lattice, positions, cotangent, filters):
    natom, width = cotangent.shape
    rows = -(-9 * (natom // width) // 8) * 8
    outs = [shape((natom + rows, width), bf16), shape((8, width), f32), shape(filters.shape, f32)]
    if keep:
        outs = [pltpu.VMEM(v.shape, v.dtype) for v in outs]
    return pl.pallas_call(
        pack_body,
        out_shape=outs,
        in_specs=[pl.BlockSpec(memory_space=pl.ANY)] * 4,
        out_specs=full_spec(3),
        scratch_shapes=[
            pltpu.VMEM(lattice.shape, lattice.dtype),
            pltpu.VMEM(positions.shape, positions.dtype),
            pltpu.SemaphoreType.DMA((3 + PIECES,)),
        ],
    )(lattice, positions, cotangent, filters)


def join_body(own_ref, got_ref, out_ref):
    out_ref[0:8, :] = own_ref[...]
    out_ref[8:16, :] = got_ref[...]


def table_body(nk, lat_ref, out_ref):
    for h in range(2):
        out_ref[h * nk : (h + 1) * nk, :] = lat_ref[8 * h : 8 * (h + 1), :].T[0:nk]


def coordinates(block, natom):
    rows = block[natom:, :].astype(f32)
    chunks = natom // block.shape[1]
    out = []
    for d in range(3):
        pieces = []
        for j in range(chunks):
            at = [9 * j + 3 * p + d for p in range(3)]
            pieces.append((rows[at[0] : at[0] + 1] + rows[at[1] : at[1] + 1]) + rows[at[2] : at[2] + 1])
        out.append(jnp.concatenate(pieces, 1))
    return out


def factor_body(natom, nk, pairs, blocks, started, last, *refs):
    atoms = sorted({z for z, t in pairs})
    zb, refs = dict(zip(atoms, refs)), refs[len(atoms) :]
    tables, refs = dict(zip(blocks, refs)), refs[len(blocks) :]
    before, refs = (dict(zip(blocks, refs)), refs[len(blocks) :]) if started else ({}, refs)
    tiles, outs = dict(zip(pairs, refs)), refs[len(pairs) :]
    where = {z: coordinates(ref, natom) for z, ref in zb.items()}

    def phase(z, t, i):
        at = (t % 2) * nk + i
        cols = [tables[t][at : at + step, d : d + 1] for d in range(3)]
        return cols[0] * where[z][0] + cols[1] * where[z][1] + cols[2] * where[z][2]

    cot = {z: ref[0:natom, :] for z, ref in zb.items()}
    step = 32
    for b, t in enumerate(blocks):
        for i in range(0, nk, step):
            sums = [None, None]
            for z in atoms:
                for k, value in enumerate(cos_sin(phase(z, t, i))):
                    value = value.astype(bf16)
                    tiles[z, t][k * nk + i : k * nk + i + step, :] = value
                    part = jnp.dot(value, cot[z], preferred_element_type=f32)
                    sums[k] = part if sums[k] is None else sums[k] + part
            for k, total in enumerate(sums):
                row = k * nk + i
                if started:
                    total = total + before[t][row : row + step, :]
                if last:
                    outs[0][2 * nk * b + row : 2 * nk * b + row + step, :] = total.astype(outs[0].dtype)
                else:
                    outs[b][row : row + step, :] = total


def shuffled(ref, flip, half, nk):
    rows = [ref[2 * nk * (t ^ flip) : 2 * nk * ((t ^ flip) + 1), :] for t in range(half)]
    return jnp.concatenate(rows, 0).astype(f32)


def pair_body(own_ref, got_ref, f_ref, fb_ref):
    total = own_ref[...] + got_ref[...].astype(f32)
    f_ref[...] = total
    fb_ref[...] = total.astype(bf16)


def weight_body(half, nk, flips, scale, *refs):
    total = refs[0][...]
    for ref, flip in zip(refs[1:], flips):
        total = total + shuffled(ref, flip // 2, half, nk)
    total = total * scale
    fb = refs[1 + len(flips) : 1 + len(flips) + half]
    weight_ref, head_ref = refs[1 + len(flips) + half :]
    for t in range(half):
        fil = fb[t][...]
        rows = total[2 * nk * t : 2 * nk * (t + 1)] * jnp.concatenate([fil, fil], 0)
        weight_ref[:, 2 * nk * t : 2 * nk * (t + 1)] = rows.T.astype(bf16)
    head_ref[...] = total[0 : 2 * nk]


def part_of(weight_ref, tiles):
    tile = jnp.concatenate([ref[...] for ref in tiles], 0)
    return jnp.dot(weight_ref[...], tile, preferred_element_type=f32)


def mine_body(nz, half, weight_ref, *refs):
    for z in range(nz):
        refs[nz * half + z][...] = part_of(weight_ref, refs[z * half : (z + 1) * half])


def node_body(half, choices, *refs):
    weight_ref, refs = refs[0], refs[1:]
    out_ref = refs[-1]

    def one(part_ref, *tiles):
        total = part_ref[...] + part_of(weight_ref, tiles)
        out_ref[...] = total.astype(out_ref.dtype)

    groups = [refs[i * (half + 1) : (i + 1) * (half + 1)] for i in range(len(choices))]
    if len(choices) == 1:
        one(*groups[0])
        return
    plane = lax.axis_index("atoms")
    for planes, group in zip(choices, groups):
        taken = plane == planes[0]
        for other in planes[1:]:
            taken = taken | (plane == other)
        pl.when(taken)(lambda group=group: one(*group))


def own_body(half, head_ref, saved_ref, weight_ref, *refs):
    node_body(half, [None], weight_ref, *refs[:-1])
    grad_ref = refs[-1]
    nk = grad_ref.shape[0]
    grad_ref[...] = head_ref[0:nk] * saved_ref[0] + head_ref[nk : 2 * nk] * saved_ref[1]


def final_body(scale, *refs):
    total = refs[0][...]
    for ref in refs[1:-1]:
        total = total + ref[...].astype(f32)
    refs[-1][...] = (total * scale).T.astype(bf16)


def shape(dims, kind):
    return jax.ShapeDtypeStruct(dims, kind)


def local(lattice, positions, cotangent, filters, saved_factor):
    nz = lax.axis_size("atoms")
    nq = lax.axis_size("kvec")
    natom, width = cotangent.shape
    nk = lattice.shape[1]
    half = nq // 2
    count = half * nk
    scale_n = 1.0 / math.sqrt(natom * nz * nq)
    scale_k = 1.0 / math.sqrt(nk * nz * nq)
    keep = nz * natom * 4 * count * 2 <= VMEM_BUDGET

    def swap(value, flip):
        return lax.ppermute(value, "kvec", [(i, i ^ flip) for i in range(nq)])

    def send(value, targets):
        return lax.ppermute(value, "atoms", list(enumerate(targets)))

    def run(body, outs, *args, keep_args=keep, keep_outs=keep):
        return call(body, outs, *args, keep_args=keep_args, keep_outs=keep_outs)

    zbuf, wide, filters = pack(keep, lattice, positions, cotangent, filters)
    ring = gather_order(nz)
    flips = list(range(2, nq, 2))
    zb = {0: zbuf}
    for d in ring:
        zb[d] = send(zbuf, [(i - d) % nz for i in range(nz)])
    (cores,) = run(join_body, [shape((16, width), f32)], wide, swap(wide, 1))
    lats = [cores] + [swap(cores, s) for s in flips]
    fils = [filters] + [swap(filters, s) for s in flips]
    table = {}
    for s, lat in zip([0] + flips, lats):
        (both,) = run(lambda *refs: table_body(nk, *refs), [shape((2 * nk, 8), f32)], lat)
        table[s] = table[s + 1] = both
    mine = list(range(0, nq, 2))
    theirs = list(range(1, nq, 2))
    tiles = {}
    total = {}

    def factor(atoms, blocks, last=None):
        pairs = [(z, t) for z in sorted(atoms) for t in blocks]
        outs = [shape((2 * nk, natom), bf16)] * len(pairs)
        if last is None:
            outs += [shape((2 * nk, width), f32)] * len(blocks)
        else:
            outs.append(shape((2 * nk * len(blocks), width), last))
        started = blocks[0] in total
        args = [zb[z] for z in sorted(atoms)] + [table[t] for t in blocks] + [total[t] for t in blocks if started]
        body = lambda *refs: factor_body(natom, nk, pairs, blocks, started, last is not None, *refs)
        got = run(body, outs, *args)
        tiles.update(zip(pairs, got))
        if last is None:
            total.update(zip(blocks, got[len(pairs) :]))
        return got[-1]

    order = [0] + ring
    cut = max(1, len(order) - 2)
    early = order[: min(2, cut)]
    for z in early:
        factor([z], [0, 1])
    for t in flips:
        factor(early, [t, t + 1])
    for z in order[len(early) : cut]:
        factor([z], list(range(nq)))
    sent = factor(order[cut:], theirs, bf16)
    kept = factor(order[cut:], mine, f32)
    pair, pair16 = run(
        pair_body,
        [shape((2 * count, width), f32), shape((2 * count, width), bf16)],
        kept,
        swap(sent, 1),
    )
    got = [swap(pair16, s) for s in flips]
    weight, head = run(
        lambda *refs: weight_body(half, nk, flips, scale_n, *refs),
        [shape((width, 2 * count), bf16), shape((2 * nk, width), f32)],
        pair,
        *got,
        *fils,
    )
    other = swap(weight, 1)
    parts = run(
        lambda *refs: mine_body(nz, half, *refs),
        [shape((width, natom), f32)] * nz,
        weight,
        *[tiles[s, t] for s in order for t in mine],
    )
    parts = dict(zip(order, parts))
    landed = []
    for targets in reduce_rounds(nz):
        planes = {}
        for i, target in enumerate(targets):
            planes.setdefault((target - i) % nz, []).append(i)
        (node,) = run(
            lambda *refs: node_body(half, list(planes.values()), *refs),
            [shape((width, natom), bf16)],
            other,
            *[v for d in planes for v in [parts[d], *[tiles[d, t] for t in theirs]]],
        )
        landed.append(send(node, targets))
    own, filter_grad = run(
        lambda *refs: own_body(half, *refs),
        [shape((width, natom), f32), shape((nk, width), f32)],
        head,
        saved_factor,
        other,
        parts[0],
        *[tiles[0, t] for t in theirs],
    )
    (node_grad,) = run(
        lambda *refs: final_body(scale_k, *refs),
        [shape((natom, width), bf16)],
        own,
        *landed,
        keep_outs=False,
    )
    return (node_grad, filter_grad)


def gather_order(nz):
    return list(range(nz - 1, 0, -1))


def reduce_rounds(nz):
    ring = list(range(nz))
    if nz <= 4:
        middle = (nz + 1) // 2
        ring = sorted(ring, key=lambda z: (z % middle, z))
    place = {z: i for i, z in enumerate(ring)}
    steps = list(range(1, nz))
    if nz <= 4:
        steps.sort(key=lambda by: (min(by, nz - by), by))
    return [[ring[(place[z] + by) % nz] for z in range(nz)] for by in steps]


def solution(mesh):
    in_specs = (
        P(None, ("atoms", "kvec")),
        P(None, ("beads", "atoms", "kvec")),
        P(("beads", "atoms", "kvec"), None),
        P(("atoms", "kvec"), None),
        P(None, ("beads", "atoms", "kvec"), None),
    )
    out_specs = (P(("beads", "atoms", "kvec"), None), P(("beads", "atoms", "kvec"), None))
    return jax.shard_map(local, mesh=mesh, in_specs=in_specs, out_specs=out_specs, check_vma=False)
```

```python
import math

import jax
import jax.numpy as jnp
from jax import lax
from jax.experimental import pallas as pl
from jax.experimental.pallas import tpu as pltpu
from jax.sharding import PartitionSpec as P


f32 = jnp.float32
bf16 = jnp.bfloat16


SIN_COEF = None
COS_COEF = None


def _fit():
    import numpy as np

    n = 4001
    t = np.cos(np.pi * (np.arange(n) + 0.5) / n)
    u = (t + 1.0) * 0.125
    r = np.sqrt(u)
    root = math.sqrt(2.0)
    sin_ratio = np.where(r > 1e-9, root * np.sin(np.pi * r) / np.maximum(r, 1e-9), root * np.pi)
    cheb = np.polynomial.chebyshev.Chebyshev
    s = cheb.fit(u, sin_ratio, 4, domain=[0.0, 0.25]).convert(kind=np.polynomial.Polynomial)
    c = cheb.fit(u, root * np.cos(np.pi * r), 4, domain=[0.0, 0.25]).convert(kind=np.polynomial.Polynomial)
    return tuple(float(v) for v in s.coef), tuple(float(v) for v in c.coef)


SIN_COEF, COS_COEF = _fit()


def _horner(coef, u):
    acc = jnp.full_like(u, coef[-1])
    for value in coef[-2::-1]:
        acc = acc * u + value
    return acc


def cos_sin(phase):
    r = phase - jnp.round(phase)
    u = r * r
    s = r * _horner(SIN_COEF, u)
    c = _horner(COS_COEF, u)
    return 1.0 - s * s, s * c


def full_spec(count):
    return [pl.BlockSpec(memory_space=pltpu.VMEM)] * count


VMEM_BUDGET = 4 * 1024 * 1024
PIECES = 4


def call(body, outs, *args, keep_args=True, keep_outs=True):
    if keep_args:
        args = [pltpu.with_memory_space_constraint(arg, pltpu.VMEM) for arg in args]
    if keep_outs:
        outs = [pltpu.VMEM(v.shape, v.dtype) for v in outs]
    return pl.pallas_call(
        body,
        out_shape=outs,
        in_specs=full_spec(len(args)),
        out_specs=full_spec(len(outs)),
    )(*args)


def pack_body(lat_hbm, pos_hbm, cot_hbm, fil_hbm, out_ref, wide_ref, fil_ref, lat_ref, pos_ref, sem):
    natom, width = cot_hbm.shape
    nk = lat_ref.shape[1]
    copies = [
        pltpu.make_async_copy(pos_hbm, pos_ref, sem.at[0]),
        pltpu.make_async_copy(lat_hbm, lat_ref, sem.at[1]),
        pltpu.make_async_copy(fil_hbm, fil_ref, sem.at[2]),
    ]
    piece = natom // PIECES
    for j in range(PIECES):
        rows = pl.ds(j * piece, piece)
        copies.append(pltpu.make_async_copy(cot_hbm.at[rows], out_ref.at[rows], sem.at[3 + j]))
    for copy in copies:
        copy.start()
    copies[0].wait()
    x = pos_ref[...]
    hi = x.astype(bf16).astype(f32)
    rest = x - hi
    mid = rest.astype(bf16).astype(f32)
    low = rest - mid
    parts = jnp.concatenate([hi, mid, low], 0)
    rows = [parts[:, j * width : (j + 1) * width] for j in range(natom // width)]
    spare = out_ref.shape[0] - natom - 9 * len(rows)
    if spare:
        rows.append(jnp.zeros((spare, width), f32))
    out_ref[natom:, :] = jnp.concatenate(rows, 0).astype(bf16)
    copies[1].wait()
    row = lax.broadcasted_iota(jnp.int32, (nk, width), 0)
    col = lax.broadcasted_iota(jnp.int32, (nk, width), 1)
    spread = (row == col % nk).astype(bf16)
    lat = lat_ref[...].astype(f32).astype(bf16)
    wide = jnp.dot(lat, spread, preferred_element_type=f32)
    wide_ref[...] = jnp.concatenate([wide, wide, wide[:2]], 0)
    for copy in copies[2:]:
        copy.wait()


def pack(keep, lattice, positions, cotangent, filters):
    natom, width = cotangent.shape
    rows = -(-9 * (natom // width) // 8) * 8
    outs = [shape((natom + rows, width), bf16), shape((8, width), f32), shape(filters.shape, f32)]
    if keep:
        outs = [pltpu.VMEM(v.shape, v.dtype) for v in outs]
    return pl.pallas_call(
        pack_body,
        out_shape=outs,
        in_specs=[pl.BlockSpec(memory_space=pl.ANY)] * 4,
        out_specs=full_spec(3),
        scratch_shapes=[
            pltpu.VMEM(lattice.shape, lattice.dtype),
            pltpu.VMEM(positions.shape, positions.dtype),
            pltpu.SemaphoreType.DMA((3 + PIECES,)),
        ],
    )(lattice, positions, cotangent, filters)


def join_body(own_ref, got_ref, out_ref):
    out_ref[0:8, :] = own_ref[...]
    out_ref[8:16, :] = got_ref[...]


def table_body(nk, lat_ref, out_ref):
    for h in range(2):
        out_ref[h * nk : (h + 1) * nk, :] = lat_ref[8 * h : 8 * (h + 1), :].T[0:nk]


def coordinates(block, natom):
    rows = block[natom:, :].astype(f32)
    chunks = natom // block.shape[1]
    out = []
    for d in range(3):
        pieces = []
        for j in range(chunks):
            at = [9 * j + 3 * p + d for p in range(3)]
            pieces.append((rows[at[0] : at[0] + 1] + rows[at[1] : at[1] + 1]) + rows[at[2] : at[2] + 1])
        out.append(jnp.concatenate(pieces, 1))
    return out


def factor_body(natom, nk, pairs, blocks, started, last, *refs):
    atoms = sorted({z for z, t in pairs})
    zb, refs = dict(zip(atoms, refs)), refs[len(atoms) :]
    tables, refs = dict(zip(blocks, refs)), refs[len(blocks) :]
    before, refs = (dict(zip(blocks, refs)), refs[len(blocks) :]) if started else ({}, refs)
    tiles, outs = dict(zip(pairs, refs)), refs[len(pairs) :]
    where = {z: coordinates(ref, natom) for z, ref in zb.items()}

    def phase(z, t, i):
        at = (t % 2) * nk + i
        cols = [tables[t][at : at + step, d : d + 1] for d in range(3)]
        return cols[0] * where[z][0] + cols[1] * where[z][1] + cols[2] * where[z][2]

    cot = {z: ref[0:natom, :] for z, ref in zb.items()}
    step = 32
    for b, t in enumerate(blocks):
        for i in range(0, nk, step):
            sums = [None, None]
            for z in atoms:
                for k, value in enumerate(cos_sin(phase(z, t, i))):
                    value = value.astype(bf16)
                    tiles[z, t][k * nk + i : k * nk + i + step, :] = value
                    part = jnp.dot(value, cot[z], preferred_element_type=f32)
                    sums[k] = part if sums[k] is None else sums[k] + part
            for k, total in enumerate(sums):
                row = k * nk + i
                if started:
                    total = total + before[t][row : row + step, :]
                if last:
                    outs[0][2 * nk * b + row : 2 * nk * b + row + step, :] = total.astype(outs[0].dtype)
                else:
                    outs[b][row : row + step, :] = total


def shuffled(ref, flip, half, nk):
    rows = [ref[2 * nk * (t ^ flip) : 2 * nk * ((t ^ flip) + 1), :] for t in range(half)]
    return jnp.concatenate(rows, 0).astype(f32)


def pair_body(own_ref, got_ref, f_ref, fb_ref):
    total = own_ref[...] + got_ref[...].astype(f32)
    f_ref[...] = total
    fb_ref[...] = total.astype(bf16)


def weight_body(half, nk, flips, scale, *refs):
    total = refs[0][...]
    for ref, flip in zip(refs[1:], flips):
        total = total + shuffled(ref, flip // 2, half, nk)
    total = total * scale
    fb = refs[1 + len(flips) : 1 + len(flips) + half]
    weight_ref, head_ref = refs[1 + len(flips) + half :]
    for t in range(half):
        fil = fb[t][...]
        rows = total[2 * nk * t : 2 * nk * (t + 1)] * jnp.concatenate([fil, fil], 0)
        weight_ref[:, 2 * nk * t : 2 * nk * (t + 1)] = rows.T.astype(bf16)
    head_ref[...] = total[0 : 2 * nk]


def part_of(weight_ref, tiles):
    tile = jnp.concatenate([ref[...] for ref in tiles], 0)
    return jnp.dot(weight_ref[...], tile, preferred_element_type=f32)


def mine_body(nz, half, weight_ref, *refs):
    for z in range(nz):
        refs[nz * half + z][...] = part_of(weight_ref, refs[z * half : (z + 1) * half])


def node_body(half, choices, *refs):
    weight_ref, refs = refs[0], refs[1:]
    out_ref = refs[-1]

    def one(part_ref, *tiles):
        total = part_ref[...] + part_of(weight_ref, tiles)
        out_ref[...] = total.astype(out_ref.dtype)

    groups = [refs[i * (half + 1) : (i + 1) * (half + 1)] for i in range(len(choices))]
    if len(choices) == 1:
        one(*groups[0])
        return
    plane = lax.axis_index("atoms")
    for planes, group in zip(choices, groups):
        taken = plane == planes[0]
        for other in planes[1:]:
            taken = taken | (plane == other)
        pl.when(taken)(lambda group=group: one(*group))


def own_body(half, head_ref, saved_ref, weight_ref, *refs):
    node_body(half, [None], weight_ref, *refs[:-1])
    grad_ref = refs[-1]
    nk = grad_ref.shape[0]
    grad_ref[...] = head_ref[0:nk] * saved_ref[0] + head_ref[nk : 2 * nk] * saved_ref[1]


def final_body(scale, *refs):
    total = refs[0][...]
    for ref in refs[1:-1]:
        total = total + ref[...].astype(f32)
    refs[-1][...] = (total * scale).T.astype(bf16)


def shape(dims, kind):
    return jax.ShapeDtypeStruct(dims, kind)


def local(lattice, positions, cotangent, filters, saved_factor):
    nz = lax.axis_size("atoms")
    nq = lax.axis_size("kvec")
    natom, width = cotangent.shape
    nk = lattice.shape[1]
    half = nq // 2
    count = half * nk
    scale_n = 1.0 / math.sqrt(natom * nz * nq)
    scale_k = 1.0 / math.sqrt(nk * nz * nq)
    keep = nz * natom * 4 * count * 2 <= VMEM_BUDGET

    def swap(value, flip):
        return lax.ppermute(value, "kvec", [(i, i ^ flip) for i in range(nq)])

    def send(value, targets):
        return lax.ppermute(value, "atoms", list(enumerate(targets)))

    def run(body, outs, *args, keep_args=keep, keep_outs=keep):
        return call(body, outs, *args, keep_args=keep_args, keep_outs=keep_outs)

    zbuf, wide, filters = pack(keep, lattice, positions, cotangent, filters)
    ring = gather_order(nz)
    flips = list(range(2, nq, 2))
    zb = {0: zbuf}
    for d in ring:
        zb[d] = send(zbuf, ring_shift(nz, -d))
    (cores,) = run(join_body, [shape((16, width), f32)], wide, swap(wide, 1))
    lats = [cores] + [swap(cores, s) for s in flips]
    fils = [filters] + [swap(filters, s) for s in flips]
    table = {}
    for s, lat in zip([0] + flips, lats):
        (both,) = run(lambda *refs: table_body(nk, *refs), [shape((2 * nk, 8), f32)], lat)
        table[s] = table[s + 1] = both
    mine = list(range(0, nq, 2))
    theirs = list(range(1, nq, 2))
    tiles = {}
    total = {}

    def factor(atoms, blocks, last=None):
        pairs = [(z, t) for z in sorted(atoms) for t in blocks]
        outs = [shape((2 * nk, natom), bf16)] * len(pairs)
        if last is None:
            outs += [shape((2 * nk, width), f32)] * len(blocks)
        else:
            outs.append(shape((2 * nk * len(blocks), width), last))
        started = blocks[0] in total
        args = [zb[z] for z in sorted(atoms)] + [table[t] for t in blocks] + [total[t] for t in blocks if started]
        body = lambda *refs: factor_body(natom, nk, pairs, blocks, started, last is not None, *refs)
        got = run(body, outs, *args)
        tiles.update(zip(pairs, got))
        if last is None:
            total.update(zip(blocks, got[len(pairs) :]))
        return got[-1]

    order = [0] + ring
    cut = max(1, len(order) - 2)
    early = order[: min(2, cut)]
    for z in early:
        factor([z], [0, 1])
    for t in flips:
        factor(early, [t, t + 1])
    for z in order[len(early) : cut]:
        factor([z], list(range(nq)))
    sent = factor(order[cut:], theirs, bf16)
    kept = factor(order[cut:], mine, f32)
    pair, pair16 = run(
        pair_body,
        [shape((2 * count, width), f32), shape((2 * count, width), bf16)],
        kept,
        swap(sent, 1),
    )
    got = [swap(pair16, s) for s in flips]
    weight, head = run(
        lambda *refs: weight_body(half, nk, flips, scale_n, *refs),
        [shape((width, 2 * count), bf16), shape((2 * nk, width), f32)],
        pair,
        *got,
        *fils,
    )
    other = swap(weight, 1)
    parts = run(
        lambda *refs: mine_body(nz, half, *refs),
        [shape((width, natom), f32)] * nz,
        weight,
        *[tiles[s, t] for s in order for t in mine],
    )
    parts = dict(zip(order, parts))
    landed = []
    for k in range(nz - 1):
        targets = ring_shift(nz, k + 1)
        planes = {k + 1: None}
        (node,) = run(
            lambda *refs: node_body(half, list(planes.values()), *refs),
            [shape((width, natom), bf16)],
            other,
            *[v for d in planes for v in [parts[d], *[tiles[d, t] for t in theirs]]],
        )
        landed.append(send(node, targets))
    own, filter_grad = run(
        lambda *refs: own_body(half, *refs),
        [shape((width, natom), f32), shape((nk, width), f32)],
        head,
        saved_factor,
        other,
        parts[0],
        *[tiles[0, t] for t in theirs],
    )
    (node_grad,) = run(
        lambda *refs: final_body(scale_k, *refs),
        [shape((natom, width), bf16)],
        own,
        *landed,
        keep_outs=False,
    )
    return (node_grad, filter_grad)


def gather_order(nz):
    return sorted(range(1, nz), key=lambda d: (-min(d, nz - d), d))


def ring_shift(nz, by):
    ring = list(range(nz))
    if nz <= 4:
        ring = ring[:1] + ring[1::2] + ring[2::2][::-1]
    place = {z: i for i, z in enumerate(ring)}
    return [ring[(place[z] + by) % nz] for z in range(nz)]


def solution(mesh):
    in_specs = (
        P(None, ("atoms", "kvec")),
        P(None, ("beads", "atoms", "kvec")),
        P(("beads", "atoms", "kvec"), None),
        P(("atoms", "kvec"), None),
        P(None, ("beads", "atoms", "kvec"), None),
    )
    out_specs = (P(("beads", "atoms", "kvec"), None), P(("beads", "atoms", "kvec"), None))
    return jax.shard_map(local, mesh=mesh, in_specs=in_specs, out_specs=out_specs, check_vma=False)
```

```python
import math

import jax
import jax.numpy as jnp
from jax import lax
from jax.experimental import pallas as pl
from jax.experimental.pallas import tpu as pltpu
from jax.sharding import PartitionSpec as P


f32 = jnp.float32
bf16 = jnp.bfloat16


SIN_COEF = None
COS_COEF = None


def _fit():
    import numpy as np

    n = 4001
    t = np.cos(np.pi * (np.arange(n) + 0.5) / n)
    u = (t + 1.0) * 0.125
    r = np.sqrt(u)
    root = math.sqrt(2.0)
    sin_ratio = np.where(r > 1e-9, root * np.sin(np.pi * r) / np.maximum(r, 1e-9), root * np.pi)
    cheb = np.polynomial.chebyshev.Chebyshev
    s = cheb.fit(u, sin_ratio, 4, domain=[0.0, 0.25]).convert(kind=np.polynomial.Polynomial)
    c = cheb.fit(u, root * np.cos(np.pi * r), 4, domain=[0.0, 0.25]).convert(kind=np.polynomial.Polynomial)
    return tuple(float(v) for v in s.coef), tuple(float(v) for v in c.coef)


SIN_COEF, COS_COEF = _fit()


def _horner(coef, u):
    acc = jnp.full_like(u, coef[-1])
    for value in coef[-2::-1]:
        acc = acc * u + value
    return acc


def cos_sin(phase):
    r = phase - jnp.round(phase)
    u = r * r
    s = r * _horner(SIN_COEF, u)
    c = _horner(COS_COEF, u)
    return 1.0 - s * s, s * c


def full_spec(count):
    return [pl.BlockSpec(memory_space=pltpu.VMEM)] * count


VMEM_BUDGET = 4 * 1024 * 1024
PIECES = 4


def call(body, outs, *args, keep_args=True, keep_outs=True):
    if keep_args:
        args = [pltpu.with_memory_space_constraint(arg, pltpu.VMEM) for arg in args]
    if keep_outs:
        outs = [pltpu.VMEM(v.shape, v.dtype) for v in outs]
    return pl.pallas_call(
        body,
        out_shape=outs,
        in_specs=full_spec(len(args)),
        out_specs=full_spec(len(outs)),
    )(*args)


def pack_body(lat_hbm, pos_hbm, cot_hbm, fil_hbm, out_ref, wide_ref, fil_ref, lat_ref, pos_ref, sem):
    natom, width = cot_hbm.shape
    nk = lat_ref.shape[1]
    copies = [
        pltpu.make_async_copy(pos_hbm, pos_ref, sem.at[0]),
        pltpu.make_async_copy(lat_hbm, lat_ref, sem.at[1]),
        pltpu.make_async_copy(fil_hbm, fil_ref, sem.at[2]),
    ]
    piece = natom // PIECES
    for j in range(PIECES):
        rows = pl.ds(j * piece, piece)
        copies.append(pltpu.make_async_copy(cot_hbm.at[rows], out_ref.at[rows], sem.at[3 + j]))
    for copy in copies:
        copy.start()
    copies[0].wait()
    x = pos_ref[...]
    hi = x.astype(bf16).astype(f32)
    rest = x - hi
    mid = rest.astype(bf16).astype(f32)
    low = rest - mid
    parts = jnp.concatenate([hi, mid, low], 0)
    rows = [parts[:, j * width : (j + 1) * width] for j in range(natom // width)]
    spare = out_ref.shape[0] - natom - 9 * len(rows)
    if spare:
        rows.append(jnp.zeros((spare, width), f32))
    out_ref[natom:, :] = jnp.concatenate(rows, 0).astype(bf16)
    copies[1].wait()
    row = lax.broadcasted_iota(jnp.int32, (nk, width), 0)
    col = lax.broadcasted_iota(jnp.int32, (nk, width), 1)
    spread = (row == col % nk).astype(bf16)
    lat = lat_ref[...].astype(f32).astype(bf16)
    wide = jnp.dot(lat, spread, preferred_element_type=f32)
    wide_ref[...] = jnp.concatenate([wide, wide, wide[:2]], 0)
    for copy in copies[2:]:
        copy.wait()


def pack(keep, lattice, positions, cotangent, filters):
    natom, width = cotangent.shape
    rows = -(-9 * (natom // width) // 8) * 8
    outs = [shape((natom + rows, width), bf16), shape((8, width), f32), shape(filters.shape, f32)]
    if keep:
        outs = [pltpu.VMEM(v.shape, v.dtype) for v in outs]
    return pl.pallas_call(
        pack_body,
        out_shape=outs,
        in_specs=[pl.BlockSpec(memory_space=pl.ANY)] * 4,
        out_specs=full_spec(3),
        scratch_shapes=[
            pltpu.VMEM(lattice.shape, lattice.dtype),
            pltpu.VMEM(positions.shape, positions.dtype),
            pltpu.SemaphoreType.DMA((3 + PIECES,)),
        ],
    )(lattice, positions, cotangent, filters)


def join_body(own_ref, got_ref, out_ref):
    out_ref[0:8, :] = own_ref[...]
    out_ref[8:16, :] = got_ref[...]


def table_body(nk, lat_ref, out_ref):
    for h in range(2):
        out_ref[h * nk : (h + 1) * nk, :] = lat_ref[8 * h : 8 * (h + 1), :].T[0:nk]


def coordinates(block, natom):
    rows = block[natom:, :].astype(f32)
    chunks = natom // block.shape[1]
    out = []
    for d in range(3):
        pieces = []
        for j in range(chunks):
            at = [9 * j + 3 * p + d for p in range(3)]
            pieces.append((rows[at[0] : at[0] + 1] + rows[at[1] : at[1] + 1]) + rows[at[2] : at[2] + 1])
        out.append(jnp.concatenate(pieces, 1))
    return out


def factor_body(natom, nk, pairs, blocks, started, last, *refs):
    atoms = sorted({z for z, t in pairs})
    zb, refs = dict(zip(atoms, refs)), refs[len(atoms) :]
    tables, refs = dict(zip(blocks, refs)), refs[len(blocks) :]
    before, refs = (dict(zip(blocks, refs)), refs[len(blocks) :]) if started else ({}, refs)
    tiles, outs = dict(zip(pairs, refs)), refs[len(pairs) :]
    where = {z: coordinates(ref, natom) for z, ref in zb.items()}

    def phase(z, t, i):
        at = (t % 2) * nk + i
        cols = [tables[t][at : at + step, d : d + 1] for d in range(3)]
        return cols[0] * where[z][0] + cols[1] * where[z][1] + cols[2] * where[z][2]

    cot = {z: ref[0:natom, :] for z, ref in zb.items()}
    step = 32
    for b, t in enumerate(blocks):
        for i in range(0, nk, step):
            sums = [None, None]
            for z in atoms:
                for k, value in enumerate(cos_sin(phase(z, t, i))):
                    value = value.astype(bf16)
                    tiles[z, t][k * nk + i : k * nk + i + step, :] = value
                    part = jnp.dot(value, cot[z], preferred_element_type=f32)
                    sums[k] = part if sums[k] is None else sums[k] + part
            for k, total in enumerate(sums):
                row = k * nk + i
                if started:
                    total = total + before[t][row : row + step, :]
                if last:
                    outs[0][2 * nk * b + row : 2 * nk * b + row + step, :] = total.astype(outs[0].dtype)
                else:
                    outs[b][row : row + step, :] = total


def shuffled(ref, flip, half, nk):
    rows = [ref[2 * nk * (t ^ flip) : 2 * nk * ((t ^ flip) + 1), :] for t in range(half)]
    return jnp.concatenate(rows, 0).astype(f32)


def pair_body(own_ref, got_ref, f_ref, fb_ref):
    total = own_ref[...] + got_ref[...].astype(f32)
    f_ref[...] = total
    fb_ref[...] = total.astype(bf16)


def weight_body(half, nk, flips, scale, *refs):
    total = refs[0][...]
    for ref, flip in zip(refs[1:], flips):
        total = total + shuffled(ref, flip // 2, half, nk)
    total = total * scale
    fb = refs[1 + len(flips) : 1 + len(flips) + half]
    weight_ref, head_ref = refs[1 + len(flips) + half :]
    for t in range(half):
        fil = fb[t][...]
        rows = total[2 * nk * t : 2 * nk * (t + 1)] * jnp.concatenate([fil, fil], 0)
        weight_ref[:, 2 * nk * t : 2 * nk * (t + 1)] = rows.T.astype(bf16)
    head_ref[...] = total[0 : 2 * nk]


def part_of(weight_ref, tiles):
    tile = jnp.concatenate([ref[...] for ref in tiles], 0)
    return jnp.dot(weight_ref[...], tile, preferred_element_type=f32)


def mine_body(nz, half, weight_ref, *refs):
    for z in range(nz):
        refs[nz * half + z][...] = part_of(weight_ref, refs[z * half : (z + 1) * half])


def node_body(half, choices, *refs):
    weight_ref, refs = refs[0], refs[1:]
    out_ref = refs[-1]

    def one(part_ref, *tiles):
        total = part_ref[...] + part_of(weight_ref, tiles)
        out_ref[...] = total.astype(out_ref.dtype)

    groups = [refs[i * (half + 1) : (i + 1) * (half + 1)] for i in range(len(choices))]
    if len(choices) == 1:
        one(*groups[0])
        return
    plane = lax.axis_index("atoms")
    for planes, group in zip(choices, groups):
        taken = plane == planes[0]
        for other in planes[1:]:
            taken = taken | (plane == other)
        pl.when(taken)(lambda group=group: one(*group))


def own_body(half, head_ref, saved_ref, weight_ref, *refs):
    node_body(half, [None], weight_ref, *refs[:-1])
    grad_ref = refs[-1]
    nk = grad_ref.shape[0]
    grad_ref[...] = head_ref[0:nk] * saved_ref[0] + head_ref[nk : 2 * nk] * saved_ref[1]


def final_body(scale, *refs):
    total = refs[0][...]
    for ref in refs[1:-1]:
        total = total + ref[...].astype(f32)
    refs[-1][...] = (total * scale).T.astype(bf16)


def shape(dims, kind):
    return jax.ShapeDtypeStruct(dims, kind)


def local(lattice, positions, cotangent, filters, saved_factor):
    nz = lax.axis_size("atoms")
    nq = lax.axis_size("kvec")
    natom, width = cotangent.shape
    nk = lattice.shape[1]
    half = nq // 2
    count = half * nk
    scale_n = 1.0 / math.sqrt(natom * nz * nq)
    scale_k = 1.0 / math.sqrt(nk * nz * nq)
    keep = nz * natom * 4 * count * 2 <= VMEM_BUDGET

    def swap(value, flip):
        return lax.ppermute(value, "kvec", [(i, i ^ flip) for i in range(nq)])

    def send(value, targets):
        return lax.ppermute(value, "atoms", list(enumerate(targets)))

    def run(body, outs, *args, keep_args=keep, keep_outs=keep):
        return call(body, outs, *args, keep_args=keep_args, keep_outs=keep_outs)

    zbuf, wide, filters = pack(keep, lattice, positions, cotangent, filters)
    ring = gather_order(nz)
    flips = list(range(2, nq, 2))
    zb = {0: zbuf}
    for d in ring:
        zb[d] = send(zbuf, [(i - d) % nz for i in range(nz)])
    (cores,) = run(join_body, [shape((16, width), f32)], wide, swap(wide, 1))
    lats = [cores] + [swap(cores, s) for s in flips]
    fils = [filters] + [swap(filters, s) for s in flips]
    table = {}
    for s, lat in zip([0] + flips, lats):
        (both,) = run(lambda *refs: table_body(nk, *refs), [shape((2 * nk, 8), f32)], lat)
        table[s] = table[s + 1] = both
    mine = list(range(0, nq, 2))
    theirs = list(range(1, nq, 2))
    tiles = {}
    total = {}

    def factor(atoms, blocks, last=None):
        pairs = [(z, t) for z in sorted(atoms) for t in blocks]
        outs = [shape((2 * nk, natom), bf16)] * len(pairs)
        if last is None:
            outs += [shape((2 * nk, width), f32)] * len(blocks)
        else:
            outs.append(shape((2 * nk * len(blocks), width), last))
        started = blocks[0] in total
        args = [zb[z] for z in sorted(atoms)] + [table[t] for t in blocks] + [total[t] for t in blocks if started]
        body = lambda *refs: factor_body(natom, nk, pairs, blocks, started, last is not None, *refs)
        got = run(body, outs, *args)
        tiles.update(zip(pairs, got))
        if last is None:
            total.update(zip(blocks, got[len(pairs) :]))
        return got[-1]

    order = [0] + ring
    cut = max(1, len(order) - 2)
    early = order[: min(2, cut)]
    for z in early:
        factor([z], [0, 1])
    for t in flips:
        factor(early, [t + 1])
    between = order[len(early) : cut]
    if between:
        for t in flips:
            factor(early, [t])
    for z in between:
        factor([z], list(range(nq)))
    sent = factor(order[cut:], theirs, bf16)
    for t in flips if not between else []:
        factor(early, [t])
    kept = factor(order[cut:], mine, f32)
    pair, pair16 = run(
        pair_body, [shape((2 * count, width), f32), shape((2 * count, width), bf16)], kept, swap(sent, 1)
    )
    got = [swap(pair16, s) for s in flips]
    weight, head = run(
        lambda *refs: weight_body(half, nk, flips, scale_n, *refs),
        [shape((width, 2 * count), bf16), shape((2 * nk, width), f32)],
        pair,
        *got,
        *fils,
    )
    other = swap(weight, 1)
    parts = run(
        lambda *refs: mine_body(nz, half, *refs),
        [shape((width, natom), f32)] * nz,
        weight,
        *[tiles[s, t] for s in order for t in mine],
    )
    parts = dict(zip(order, parts))
    landed = []
    for targets in reduce_rounds(nz):
        planes = {}
        for i, target in enumerate(targets):
            planes.setdefault((target - i) % nz, []).append(i)
        (node,) = run(
            lambda *refs: node_body(half, list(planes.values()), *refs),
            [shape((width, natom), bf16)],
            other,
            *[v for d in planes for v in [parts[d], *[tiles[d, t] for t in theirs]]],
        )
        landed.append(send(node, targets))
    own, filter_grad = run(
        lambda *refs: own_body(half, *refs),
        [shape((width, natom), f32), shape((nk, width), f32)],
        head,
        saved_factor,
        other,
        parts[0],
        *[tiles[0, t] for t in theirs],
    )
    (node_grad,) = run(
        lambda *refs: final_body(scale_k, *refs), [shape((natom, width), bf16)], own, *landed, keep_outs=False
    )
    return (node_grad, filter_grad)


def gather_order(nz):
    return list(range(nz - 1, 0, -1))


def reduce_rounds(nz):
    ring = list(range(nz))
    if nz <= 4:
        ring = ring[:1] + ring[1::2] + ring[2::2][::-1]
    place = {z: i for i, z in enumerate(ring)}
    return [[ring[(place[z] + by) % nz] for z in range(nz)] for by in range(1, nz)]


def solution(mesh):
    in_specs = (
        P(None, ("atoms", "kvec")),
        P(None, ("beads", "atoms", "kvec")),
        P(("beads", "atoms", "kvec"), None),
        P(("atoms", "kvec"), None),
        P(None, ("beads", "atoms", "kvec"), None),
    )
    out_specs = (P(("beads", "atoms", "kvec"), None), P(("beads", "atoms", "kvec"), None))
    return jax.shard_map(local, mesh=mesh, in_specs=in_specs, out_specs=out_specs, check_vma=False)
```
